1024 devices in a mesh: gx: 32 (over y, x), gy: 8 (over z_lo), gz: 4 (over z_hi, core).
Axes of the slice: x: 4, y: 8, z: 16 (z_hi: 2, z_lo: 8; z = z_hi * 8 + z_lo), core: 2. Of those that a mesh axis runs over, the one named last changes fastest.
Arguments:
- pair_blocks: float32 [529, 32768], P(None, ('gx', 'gy', 'gz')), may hold values from -6 to 6
- basis_map: float32 [529, 64], replicated, may hold values from -0.25 to 0.25
- pair_cells: int32 [3, 32768], P(None, ('gx', 'gy', 'gz')), may hold values from 0 to 511, as said below
- pair_offsets: float32 [3, 32768], P(None, ('gx', 'gy', 'gz')), may hold values from 0 to 1
- exponent_index: int32 [32768], P(('gx', 'gy', 'gz')), may hold values from 0 to 15
- radius_index: int32 [32768], P(('gx', 'gy', 'gz')), may hold values from 0 to 4
- exponents: float32 [16], replicated, may hold values from 7 to 9
Outputs:
- density: float32 [256, 256, 512], P('gx', 'gy', 'gz')
- spectrum: float32 [2, 512, 256, 256], P(None, ('gy', 'gz'), 'gx')
The draws below stay inside these ranges and needn't reach their ends.
Inputs may be any that keep to these rules, and one draw needn't show every extreme that they name: The y of pair_cells column p lies among the 32 cells, and its z among the 128 cells, of the gy and gz index of the device that holds column p. Of the pairs that one device holds at most 2 have x in the same run of 8 cells that one gx index holds, and in every draw some such run gets exactly 2 from every device.
All inputs are finite; a program needn't handle non-finite values.
Results may differ from the reference program's by a relative error of at most 0.0003.
Values sent between devices are 32-bit elements; how exact they have to be, the bound alone decides.
A program may use at most 32 MiB of HBM per device.

```python
import math
import jax
import jax.numpy as jnp
from jax import lax

BLOCK = 23
DEG = 3
NPOLY = 64
NEXP = 16
HALO = 8
CX = 8
CY = 32
CZ = 128
PAIR_DEV = 32
CAP = 2
PAIRS = 32768
NX = 256
NY = 256
NZ = 512
N_GX = 32
N_GY = 8
N_GZ = 4


def draw_pair_cells(key, part):
    source_count = N_GX * N_GY * N_GZ
    slot_count = N_GX * CAP
    key_level, key_top, key_pick, key_perm, key_x, key_y, key_z = jax.random.split(key, 7)
    levels = jax.random.randint(key_level, (N_GX,), 0, 4)
    favourite = jax.random.randint(key_top, (), 0, N_GX)
    levels = jnp.where(jnp.arange(N_GX) == favourite, 4, levels)
    sources = jnp.arange(source_count, dtype=jnp.int32)
    slot_ids = jnp.arange(slot_count, dtype=jnp.int32)
    slot_target = slot_ids // CAP
    first_slot = slot_ids % CAP == 0
    edge_class = (slot_target[None, :] + sources[:, None]) % 4
    upper_edge = first_slot[None, :] & (edge_class == 0)
    lower_edge = first_slot[None, :] & (edge_class == 2)
    slot_levels = jnp.where(upper_edge | lower_edge, 5, levels[slot_target][None, :])
    noise = jax.random.randint(key_pick, (source_count, slot_count), 0, 65536)
    scores = (slot_levels * 65536 + noise) * slot_count + slot_ids[None, :]
    unused, chosen = lax.top_k(scores, PAIR_DEV)
    orders = jax.vmap(lambda sub_key: jax.random.permutation(sub_key, PAIR_DEV))(jax.random.split(key_perm, source_count))
    chosen = jnp.take_along_axis(chosen, orders, 1)
    targets = chosen // CAP
    chosen_upper = jnp.take_along_axis(upper_edge, chosen, 1)
    chosen_lower = jnp.take_along_axis(lower_edge, chosen, 1)
    source_y = sources // N_GZ % N_GY
    source_z = sources % N_GZ
    inner_x = jax.random.randint(key_x, (source_count, PAIR_DEV), 0, CX)
    inner_x = jnp.where(chosen_upper, CX - 1, jnp.where(chosen_lower, 0, inner_x))
    cells_x = targets * CX + inner_x
    cells_y = source_y[:, None] * CY + jax.random.randint(key_y, (source_count, PAIR_DEV), 0, CY)
    cells_z = source_z[:, None] * CZ + jax.random.randint(key_z, (source_count, PAIR_DEV), 0, CZ)
    return jnp.stack([cells_x, cells_y, cells_z]).reshape(3, source_count * PAIR_DEV).astype(jnp.int32)


def set_ends(entries, own_key, low, high):
    extent = entries.shape
    place = [jax.random.randint(jax.random.fold_in(own_key, axis), (), 0, extent[axis]) for axis in range(len(extent))]
    entries = entries.at[tuple(place)].set(low)
    longest = extent.index(max(extent))
    place[longest] = (place[longest] + 1) % extent[longest]
    return entries.at[tuple(place)].set(high)


def steps_of(stream_key, dims, cuts, low, largest):
    level = 1.0
    for position, blocks in cuts:
        steps = jax.random.uniform(jax.random.fold_in(jax.random.fold_in(stream_key, 6), position), (blocks,), jnp.float32, low / len(cuts), largest / len(cuts))
        level = level * jnp.repeat(jnp.exp(steps), dims[position] // blocks).reshape((-1,) + (1,) * (len(dims) - 1 - position))
    return level


def centred(rng, dims, scale, limit, shards=(), kind=jnp.bfloat16):
    factor_of = steps_of(rng, dims, shards, -0.22, 0.18) if shards else 1.0
    entries = jax.random.normal(rng, dims, jnp.float32) * scale * factor_of
    return jnp.minimum(jnp.maximum(entries, -limit), limit).astype(kind)


def setup_inputs(seed: int = 0) -> dict:
    seeds = jax.random.split(jax.random.key(seed), 8)
    pair_blocks = centred(seeds[0], (BLOCK * BLOCK, PAIRS), 1.0, 6.0, ((1, 1024),), jnp.float32)
    basis_map = centred(seeds[1], (BLOCK * BLOCK, NPOLY), (BLOCK * BLOCK) ** -0.5, 0.25, (), jnp.float32)
    pair_cells = draw_pair_cells(jax.random.fold_in(seeds[7], 71), 0)
    pair_offsets = jnp.clip(1.0 * jax.random.uniform(seeds[3], (3, PAIRS), jnp.float32) ** steps_of(seeds[3], (3, PAIRS), ((1, 1024),), -0.2, 0.2), 0.0, 1.0)
    exponent_index = set_ends(jax.random.randint(seeds[4], (PAIRS,), 0, NEXP), jax.random.fold_in(seeds[4], 1), 0, NEXP - 1).astype(jnp.int32)
    radius_index = set_ends(jax.random.randint(seeds[5], (PAIRS,), 0, HALO // 2 + 1), jax.random.fold_in(seeds[5], 1), 0, (HALO // 2 + 1) - 1).astype(jnp.int32)
    exponents = jnp.clip(jnp.exp(jax.random.uniform(seeds[6], (NEXP,), jnp.float32, math.log(7.0), math.log(9.0))), 7.0, 9.0)
    return dict(pair_blocks=pair_blocks, basis_map=basis_map, pair_cells=pair_cells, pair_offsets=pair_offsets, exponent_index=exponent_index, radius_index=radius_index, exponents=exponents)


highest = lax.Precision.HIGHEST


def pair_factors(offsets_row, exponent_values, radius_cells):
    span = jnp.arange(2 * HALO + 1, dtype=jnp.int32) - HALO
    distance = span[None, :].astype(jnp.float32) - offsets_row[:, None]
    inside = (jnp.abs(span)[None, :] <= radius_cells[:, None]).astype(jnp.float32)
    envelope = jnp.exp(-exponent_values[:, None] * distance * distance) * inside
    scaled = distance / HALO
    return jnp.stack([scaled ** degree * envelope for degree in range(DEG + 1)], 1)


def reference(pair_blocks, basis_map, pair_cells, pair_offsets, exponent_index, radius_index, exponents):
    side = DEG + 1
    pair_total = pair_blocks.shape[1]
    group_size = 64
    group_count = pair_total // group_size
    coefficients = jnp.dot(basis_map.T, pair_blocks, precision=highest)
    radius_cells = HALO - radius_index
    radius_float = radius_cells.astype(jnp.float32)
    exponent_values = exponents[exponent_index] / (radius_float * radius_float)
    span = jnp.arange(2 * HALO + 1, dtype=jnp.int32) - HALO

    def regroup(values):
        return values.reshape((group_count, group_size) + values.shape[1:])

    pieces_all = (regroup(coefficients.T.reshape(pair_total, side, side, side)),
                  regroup(pair_factors(pair_offsets[0], exponent_values, radius_cells)),
                  regroup(pair_factors(pair_offsets[1], exponent_values, radius_cells)),
                  regroup(pair_factors(pair_offsets[2], exponent_values, radius_cells)),
                  regroup(pair_cells.T))

    def add_group(density_grid, pieces):
        pair_coefs, along_x, along_y, along_z, centre_cells = pieces
        partial_z = jnp.einsum('sijk,skc->sijc', pair_coefs, along_z, precision=highest)
        partial_y = jnp.einsum('sjb,sijc->sibc', along_y, partial_z, precision=highest)
        tile_values = jnp.einsum('sia,sibc->sabc', along_x, partial_y, precision=highest)
        rows_x = (centre_cells[:, 0:1] + span[None, :]) % NX
        rows_y = (centre_cells[:, 1:2] + span[None, :]) % NY
        rows_z = (centre_cells[:, 2:3] + span[None, :]) % NZ
        density_grid = density_grid.at[rows_x[:, :, None, None], rows_y[:, None, :, None], rows_z[:, None, None, :]].add(tile_values)
        return density_grid, None

    density, unused = lax.scan(add_group, jnp.zeros((NX, NY, NZ), jnp.float32), pieces_all)
    transform = jnp.fft.fftn(jnp.transpose(density, (2, 1, 0)), norm="ortho")
    spectrum = jnp.stack([jnp.real(transform), jnp.imag(transform)]).astype(jnp.float32)
    return density, spectrum
```

```python
import math

import jax
import jax.numpy as jnp
import ml_dtypes
import numpy as np
from jax import lax
from jax.experimental import pallas as pl
from jax.experimental.pallas import tpu as pltpu
from jax.sharding import PartitionSpec as P

HALO = 8
CX, CY, CZ = 8, 32, 128
GX, GY, GZ = 32, 8, 4
RING = GY * GZ
NZ = GZ * CZ
NXY = 256
SLOTS = GX * 8
GROUPS = 6
SLAB = 72
MESH = pl.DeviceIdType.MESH
F32 = jnp.float32
BF16 = jnp.bfloat16

NN = (((1,), (0,)), ((), ()))
NT = (((1,), (1,)), ((), ()))
TN = (((0,), (0,)), ((), ()))


def halves(value):
    high = value.astype(BF16)
    return high, (value - high.astype(F32)).astype(BF16)


def dot(a, b, dims):
    return lax.dot_general(a, b, dims, preferred_element_type=F32)


def dot3(a, b, dims):
    return dot(a[0], b[0], dims) + (dot(a[0], b[1], dims) + dot(a[1], b[0], dims))


def np_halves(value):
    value = value.astype(np.float32)
    high = value.astype(ml_dtypes.bfloat16)
    return high, (value - high.astype(np.float32)).astype(ml_dtypes.bfloat16)


def depth_matrix():
    lane = np.arange(128)
    kz = 16 * (8 * np.arange(4)[:, None] + lane[None, :] % 8) + lane[None, :] // 8
    phase = np.arange(NZ)[:, None] * kz.reshape(-1)[None, :] % NZ
    angle = phase * (2.0 * math.pi / NZ)
    scale = 1.0 / math.sqrt(NZ)
    return np.concatenate([np.cos(angle) * scale, -np.sin(angle) * scale], 1)


def plane_matrices():
    index = np.arange(NXY)
    angle = (index[:, None] * index[None, :] % NXY) * (2.0 * math.pi / NXY)
    scale = 1.0 / math.sqrt(NXY)
    return np.cos(angle) * scale, np.sin(angle) * scale


def iota(shape, axis):
    return lax.broadcasted_iota(jnp.int32, shape, axis)


def swap_lanes(v, count, group):
    bit = 1
    while bit < count:
        shift = bit * group
        v = v.reshape(count // (2 * bit), 2, bit * 8, 128)
        a = v[:, 0].reshape(count * 4, 128)
        c = v[:, 1].reshape(count * 4, 128)
        low = (iota((count * 4, 128), 1) // shift) % 2 == 0
        na = jnp.where(low, a, pltpu.roll(c, shift, 1))
        nc = jnp.where(low, pltpu.roll(a, 128 - shift, 1), c)
        parts = (count // (2 * bit), 1, bit * 8, 128)
        v = jnp.concatenate([na.reshape(parts), nc.reshape(parts)], 1)
        v = v.reshape(count, 8, 128)
        bit *= 2
    return v


def kernel(
    blocks_ref, basis_ref, cells_ref, offsets_ref, eidx_ref, ridx_ref, exps_ref,
    wz_hbm, wxy_hbm, dens_ref, spec_ref,
    wz, wxy, out1, recv1, amps, t_hi, t_lo, slabs, main_in, rim_in, lines,
    out4, in4, out5, in5, dens_in,
    wsem, s1, r1, s3, r3, r3x, s4, r4, s5, r5, sd, rd,
):
    gx, gy, gz = lax.axis_index("gx"), lax.axis_index("gy"), lax.axis_index("gz")
    me = gy * GZ + gz

    def plane_peer(target):
        return {"gx": target}

    def ring_peer(target):
        return {"gy": target // GZ, "gz": target % GZ}

    wz_copy = pltpu.make_async_copy(wz_hbm, wz, wsem.at[0])
    wxy_copy = pltpu.make_async_copy(wxy_hbm, wxy, wsem.at[1])
    wz_copy.start()
    wxy_copy.start()

    barrier = pltpu.get_barrier_semaphore()

    @pl.loop(1, GX)
    def _(d):
        pl.semaphore_signal(
            barrier, inc=1, device_id=plane_peer(lax.rem(gx + d, GX)), device_id_type=MESH
        )

    @pl.loop(1, RING)
    def _(d):
        pl.semaphore_signal(
            barrier, inc=1, device_id=ring_peer(lax.rem(me + d, RING)), device_id_type=MESH
        )

    coefs = dot3(halves(basis_ref[...]), halves(blocks_ref[...]), TN)
    cells = cells_ref[...].astype(F32)
    radius = (HALO - ridx_ref[...]).astype(F32)
    rate = jnp.zeros((1, 32), F32)
    for e in range(16):
        rate = rate + jnp.where(eidx_ref[...] == e, exps_ref[e], 0.0)
    rate = rate / (radius * radius)
    data = jnp.concatenate(
        [coefs, cells, offsets_ref[...], rate, radius, jnp.zeros((56, 32), F32)], 0
    )
    owner = cells_ref[0:1, :] // CX
    same_pair = iota((32, 32), 0) == iota((32, 32), 1)
    owner_column = jnp.sum(
        jnp.where(same_pair, owner.astype(F32), 0.0), axis=1, keepdims=True
    ).astype(jnp.int32)
    earlier = (owner_column == owner) & (iota((32, 32), 0) < iota((32, 32), 1))
    within = jnp.sum(jnp.where(earlier, 1.0, 0.0), axis=0, keepdims=True).astype(jnp.int32)
    base = owner * 2 + within
    row = iota((SLOTS, 1), 0)
    slot = row % 8
    code = (row // 8 + slot // 2 + (GX - 1)) % GX * 2 + slot % 2
    code = jnp.where(slot < 6, code, -1)
    pick = jnp.where(code == base, 1.0, 0.0).astype(BF16)
    high, middle = halves(data)
    rest = (data - high.astype(F32) - middle.astype(F32)).astype(BF16)
    routed = dot(pick, high, NT) + dot(pick, middle, NT) + dot(pick, rest, NT)
    out1[...] = routed.reshape(GX, 8, 128)
    recv1[gx] = out1[gx]

    pl.semaphore_wait(barrier, GX + RING - 2)

    def copy1(target, source):
        return pltpu.make_async_remote_copy(
            src_ref=out1.at[target], dst_ref=recv1.at[source],
            send_sem=s1.at[target], recv_sem=r1.at[source],
            device_id=plane_peer(target), device_id_type=MESH,
        )

    @pl.loop(1, GX)
    def _(d):
        copy1(lax.rem(gx + d, GX), gx).start()

    @pl.loop(1, GX)
    def _(d):
        other = lax.rem(gx + d, GX)
        copy1(other, other).wait_recv()

    table = recv1[...].reshape(SLOTS, 128).T
    cx, cy, cz = table[64:65], table[65:66], table[66:67]
    ox, oy, oz = table[67:68], table[68:69], table[69:70]
    rates, radii = table[70:71], table[71:72]

    def factors(offset_cells, offset_in):
        distance = offset_cells - offset_in
        inside = jnp.abs(offset_cells) <= radii
        envelope = jnp.where(inside, jnp.exp(-rates * distance * distance), 0.0)
        scaled = distance * (1.0 / HALO)
        first = envelope * scaled
        second = first * scaled
        return [envelope, first, second, second * scaled]

    step_x = (gx * CX + iota((CX, 1), 0)).astype(F32) - cx
    step_x = jnp.where(step_x > 128.0, step_x - 256.0, step_x)
    step_x = jnp.where(step_x < -128.0, step_x + 256.0, step_x)
    along_x = factors(step_x, ox)
    for j in range(4):
        for k in range(4):
            total = table[j * 4 + k : j * 4 + k + 1] * along_x[0]
            for i in range(1, 4):
                at = i * 16 + j * 4 + k
                total = total + table[at : at + 1] * along_x[i]
            amps[j * 4 + k] = total
    along_y = factors((gy * CY - HALO + iota((48, 1), 0)).astype(F32) - cy, oy)
    z_row = iota((256, 1), 0)
    rim = z_row % 16
    z_cell = jnp.where(
        z_row < CZ, z_row, jnp.where(rim < HALO, CZ + rim, rim - 2 * HALO)
    )
    along_z = factors((gz * CZ + z_cell).astype(F32) - cz, oz)

    for x in range(CX):
        for k in range(4):
            total = amps[k, x : x + 1, :] * along_y[0]
            for j in range(1, 4):
                total = total + amps[j * 4 + k, x : x + 1, :] * along_y[j]
            high, low = halves(total)
            t_hi[x * 48 : (x + 1) * 48, k * SLOTS : (k + 1) * SLOTS] = high
            t_lo[x * 48 : (x + 1) * 48, k * SLOTS : (k + 1) * SLOTS] = low
    z_all = halves(jnp.concatenate(along_z, 1))
    block = dot3((t_hi[...], t_lo[...]), z_all, NT)
    keep = iota((8, 128), 1) // 16 == iota((8, 128), 0)
    for x in range(CX):
        for g in range(GROUPS):
            at = x * 48 + g * 8
            slabs[g, x * 8 : (x + 1) * 8, :] = block[at : at + 8, :128]
            slabs[g, 64 + x : 65 + x, :] = jnp.sum(
                jnp.where(keep, block[at : at + 8, 128:], 0.0), axis=0, keepdims=True
            )

    def copy3(group, source):
        return pltpu.make_async_remote_copy(
            src_ref=slabs.at[group], dst_ref=main_in.at[source],
            send_sem=s3.at[group], recv_sem=r3.at[source],
            device_id={"gz": group - 1}, device_id_type=MESH,
        )

    def copy3_rim(group, source, row_to, depth_to):
        return pltpu.make_async_remote_copy(
            src_ref=slabs.at[group], dst_ref=rim_in.at[source],
            send_sem=s3.at[group], recv_sem=r3x.at[source],
            device_id={"gy": row_to, "gz": depth_to}, device_id_type=MESH,
        )

    before, after = lax.rem(gy + GY - 1, GY), lax.rem(gy + 1, GY)

    @pl.loop(1, GZ)
    def _(d):
        copy3(1 + lax.rem(gz + d, GZ), gz).start()

    copy3_rim(0, gz, before, GZ - 1).start()
    copy3_rim(5, gz, after, 0).start()
    main_in[gz] = slabs[1 + gz]

    edge = (gz == 0) | (gz == GZ - 1)

    @pl.when(jnp.logical_not(edge))
    def _():
        rim_in[...] = jnp.zeros((GZ, SLAB, 128), F32)

    wz_copy.wait()
    wxy_copy.wait()

    @pl.loop(1, GZ)
    def _(d):
        other = lax.rem(gz + d, GZ)
        copy3(1 + other, other).wait_recv()

    @pl.when(edge)
    def _():
        @pl.loop(0, GZ)
        def _(source):
            copy3_rim(0, source, before, GZ - 1).wait_recv()

    row_lane = iota((64, 128), 1)
    keep_rows = row_lane // 16 == iota((64, 128), 0) % 8
    rims = []
    for q in range(GZ):
        packed = main_in[q, 64:SLAB, :] + rim_in[q, 64:SLAB, :]
        spread = jnp.concatenate(
            [jnp.broadcast_to(packed[x : x + 1], (8, 128)) for x in range(CX)], 0
        )
        spread = jnp.where(keep_rows, spread, 0.0)
        for shift in (16, 32, 64):
            spread = spread + pltpu.roll(spread, shift, 1)
        rims.append(spread)
    for q in range(GZ):
        lines[q] = (
            main_in[q, 0:64, :]
            + rim_in[q, 0:64, :]
            + jnp.where(row_lane >= CZ - HALO, rims[(q + 1) % GZ], 0.0)
            + jnp.where(row_lane < HALO, rims[(q + GZ - 1) % GZ], 0.0)
        )
    line_parts = halves(jnp.concatenate([lines[q] for q in range(GZ)], 1))
    for c in range(8):
        columns = slice(c * 128, (c + 1) * 128)
        part = dot3(line_parts, (wz[0, :, columns], wz[1, :, columns]), NN)
        part = swap_lanes(part.reshape(8, 8, 128), 8, 1)
        first = c % 4 * 8
        out4[first : first + 8, c // 4] = part

    def copy4(target, source):
        return pltpu.make_async_remote_copy(
            src_ref=out4.at[target], dst_ref=in4.at[:, pl.ds(pl.multiple_of(source * 8, 8), 8), :],
            send_sem=s4.at[target], recv_sem=r4.at[source],
            device_id=ring_peer(target), device_id_type=MESH,
        )

    @pl.loop(1, RING)
    def _(d):
        copy4(lax.rem(me + d, RING), me).start()

    def copy_d(target, source):
        return pltpu.make_async_remote_copy(
            src_ref=lines.at[target], dst_ref=dens_in.at[source],
            send_sem=sd.at[target], recv_sem=rd.at[source],
            device_id={"gz": target}, device_id_type=MESH,
        )

    @pl.loop(1, GZ)
    def _(d):
        copy_d(lax.rem(gz + d, GZ), gz).start()

    in4[:, pl.ds(pl.multiple_of(me * 8, 8), 8), :] = out4[me]
    dens_in[gz] = lines[gz]

    @pl.loop(1, RING)
    def _(d):
        other = lax.rem(me + d, RING)
        copy4(other, other).wait_recv()

    cosines = (wxy[0], wxy[1])
    sines = (wxy[2], wxy[3])
    rows_in = halves(jnp.concatenate([in4[0], in4[1]], 1))
    with_cos = dot3(cosines, rows_in, NN)
    with_sin = dot3(sines, rows_in, NN)
    out5[0] = with_cos[:, :128] + with_sin[:, 128:]
    out5[1] = with_cos[:, 128:] - with_sin[:, :128]

    def copy5(target, source):
        return pltpu.make_async_remote_copy(
            src_ref=out5.at[:, pl.ds(pl.multiple_of(target * 8, 8), 8), :], dst_ref=in5.at[source],
            send_sem=s5.at[target], recv_sem=r5.at[source],
            device_id=plane_peer(target), device_id_type=MESH,
        )

    @pl.loop(1, GX)
    def _(d):
        copy5(lax.rem(gx + d, GX), gx).start()

    in5[gx] = out5[:, pl.ds(pl.multiple_of(gx * 8, 8), 8), :]

    @pl.loop(1, GX)
    def _(d):
        other = lax.rem(gx + d, GX)
        copy5(other, other).wait_recv()

    sides = []
    for part in range(2):
        pieces = [
            swap_lanes(in5[h * 16 : (h + 1) * 16, part], 16, 8).reshape(128, 128)
            for h in range(2)
        ]
        sides.append(jnp.concatenate(pieces, 1))
    x_lines = halves(jnp.concatenate(sides, 0))
    with_cos = dot3(x_lines, cosines, NN)
    with_sin = dot3(x_lines, sines, NN)
    spec_ref[0] = (with_cos[:128] + with_sin[128:]).reshape(16, 8, NXY)
    spec_ref[1] = (with_cos[128:] - with_sin[:128]).reshape(16, 8, NXY)

    @pl.loop(1, GZ)
    def _(d):
        other = lax.rem(gz + d, GZ)
        copy_d(other, other).wait_recv()

    for q in range(GZ):
        dens_ref[:, q * 8 : (q + 1) * 8, :] = dens_in[q].reshape(8, 8, 128)

    @pl.loop(1, GX)
    def _(d):
        other = lax.rem(gx + d, GX)
        copy1(other, gx).wait_send()
        copy5(other, gx).wait_send()

    @pl.loop(1, RING)
    def _(d):
        copy4(lax.rem(me + d, RING), me).wait_send()

    @pl.loop(1, GZ)
    def _(d):
        other = lax.rem(gz + d, GZ)
        copy3(1 + other, gz).wait_send()
        copy_d(other, gz).wait_send()

    copy3_rim(0, gz, before, GZ - 1).wait_send()
    copy3_rim(5, gz, after, 0).wait_send()


def solution(mesh):
    wz = np.stack(np_halves(depth_matrix()))
    cos_m, sin_m = plane_matrices()
    wxy = np.stack([*np_halves(cos_m), *np_halves(sin_m)])
    vmem = pl.BlockSpec(memory_space=pltpu.VMEM)
    anywhere = pl.BlockSpec(memory_space=pl.ANY)
    dma = pltpu.SemaphoreType.DMA
    call = pl.pallas_call(
        kernel,
        out_shape=(
            jax.ShapeDtypeStruct((CX, CY, CZ), F32),
            jax.ShapeDtypeStruct((2, 16, 8, NXY), F32),
        ),
        in_specs=[vmem] * 6 + [pl.BlockSpec(memory_space=pltpu.SMEM), anywhere, anywhere],
        out_specs=(vmem, vmem),
        scratch_shapes=[
            pltpu.VMEM((2, NZ, 2 * NZ), BF16),
            pltpu.VMEM((4, NXY, NXY), BF16),
            pltpu.VMEM((GX, 8, 128), F32),
            pltpu.VMEM((GX, 8, 128), F32),
            pltpu.VMEM((16, 8, SLOTS), F32),
            pltpu.VMEM((384, 4 * SLOTS), BF16),
            pltpu.VMEM((384, 4 * SLOTS), BF16),
            pltpu.VMEM((GROUPS, SLAB, 128), F32),
            pltpu.VMEM((GZ, SLAB, 128), F32),
            pltpu.VMEM((GZ, SLAB, 128), F32),
            pltpu.VMEM((GZ, 64, 128), F32),
            pltpu.VMEM((RING, 2, 8, 128), F32),
            pltpu.VMEM((2, NXY, 128), F32),
            pltpu.VMEM((2, NXY, 128), F32),
            pltpu.VMEM((GX, 2, 8, 128), F32),
            pltpu.VMEM((GZ, 64, 128), F32),
            dma((2,)),
            dma((GX,)), dma((GX,)),
            dma((GROUPS,)), dma((GZ,)), dma((GZ,)),
            dma((RING,)), dma((RING,)),
            dma((GX,)), dma((GX,)),
            dma((GZ,)), dma((GZ,)),
        ],
        compiler_params=pltpu.CompilerParams(collective_id=0, has_side_effects=True),
        name="pair_grid_transform",
    )

    def shards(blocks, basis, cells, offsets, eidx, ridx, exps):
        return call(
            blocks, basis, cells, offsets, eidx.reshape(1, -1), ridx.reshape(1, -1), exps,
            jnp.asarray(wz), jnp.asarray(wxy),
        )

    split = ("gx", "gy", "gz")
    placed = (P(None, split), P(), P(None, split), P(None, split), P(split), P(split), P())
    return jax.shard_map(
        shards,
        mesh=mesh,
        in_specs=placed,
        out_specs=(P("gx", "gy", "gz"), P(None, ("gy", "gz"), "gx", None)),
        check_vma=False,
    )
```

```python
import math

import jax
import jax.numpy as jnp
import ml_dtypes
import numpy as np
from jax import lax
from jax.experimental import pallas as pl
from jax.experimental.pallas import tpu as pltpu
from jax.sharding import PartitionSpec as P

HALO = 8
CX, CY, CZ = 8, 32, 128
GX, GY, GZ = 32, 8, 4
RING = GY * GZ
NZ = GZ * CZ
NXY = 256
SLOTS = GX * 8
GROUPS = 6
SLAB = 72
MESH = pl.DeviceIdType.MESH
F32 = jnp.float32
BF16 = jnp.bfloat16

NN = (((1,), (0,)), ((), ()))
NT = (((1,), (1,)), ((), ()))


def halves(value):
    high = value.astype(BF16)
    return high, (value - high.astype(F32)).astype(BF16)


def dot(a, b, dims):
    return lax.dot_general(a, b, dims, preferred_element_type=F32)


def dot3(a, b, dims):
    return dot(a[0], b[0], dims) + (dot(a[0], b[1], dims) + dot(a[1], b[0], dims))


def np_halves(value):
    value = value.astype(np.float32)
    high = value.astype(ml_dtypes.bfloat16)
    return high, (value - high.astype(np.float32)).astype(ml_dtypes.bfloat16)


def depth_matrix():
    lane = np.arange(128)
    kz = 16 * (8 * np.arange(4)[:, None] + lane[None, :] % 8) + lane[None, :] // 8
    phase = np.arange(NZ)[:, None] * kz.reshape(-1)[None, :] % NZ
    angle = phase * (2.0 * math.pi / NZ)
    scale = 1.0 / math.sqrt(NZ)
    return np.concatenate([np.cos(angle) * scale, -np.sin(angle) * scale], 1)


def plane_matrices():
    index = np.arange(NXY)
    angle = (index[:, None] * index[None, :] % NXY) * (2.0 * math.pi / NXY)
    scale = 1.0 / math.sqrt(NXY)
    return np.cos(angle) * scale, np.sin(angle) * scale


def iota(shape, axis):
    return lax.broadcasted_iota(jnp.int32, shape, axis)


def swap_lanes(v, count, group):
    bit = 1
    while bit < count:
        shift = bit * group
        v = v.reshape(count // (2 * bit), 2, bit * 8, 128)
        a = v[:, 0].reshape(count * 4, 128)
        c = v[:, 1].reshape(count * 4, 128)
        low = (iota((count * 4, 128), 1) // shift) % 2 == 0
        na = jnp.where(low, a, pltpu.roll(c, shift, 1))
        nc = jnp.where(low, pltpu.roll(a, 128 - shift, 1), c)
        parts = (count // (2 * bit), 1, bit * 8, 128)
        v = jnp.concatenate([na.reshape(parts), nc.reshape(parts)], 1)
        v = v.reshape(count, 8, 128)
        bit *= 2
    return v


def kernel(
    blocks_ref, basis_ref, cells_ref, offsets_ref, eidx_ref, ridx_ref, exps_ref,
    wz_hbm, wxy_hbm, dens_ref, spec_ref,
    wz, wxy, out1, recv1, amps, t_hi, t_lo, slabs, main_in, rim_in, lines,
    out4, in4, out5, in5, dens_in,
    wsem, s1, r1, s3, r3, r3x, s4, r4, s5, r5, sd, rd,
):
    gx, gy, gz = lax.axis_index("gx"), lax.axis_index("gy"), lax.axis_index("gz")
    me = gy * GZ + gz

    half, core = gz // 2, gz % 2

    def far_first(i, reach):
        return (reach - (i + 1) // 2) * (2 * (i % 2) - 1)

    def plane_step(i):
        row = lax.rem(gx // 4 + far_first(i // 4, 4) + 8, 8)
        return row * 4 + lax.rem(gx % 4 + far_first(i % 4, 2) + 4, 4)

    def ring_step(i):
        depth = lax.rem(gy + 8 * half + far_first(i // 2, 8) + 16, 16)
        return depth % 8 * GZ + depth // 8 * 2 + (core + 1 + i) % 2

    def plane_peer(target):
        return {"gx": target}

    def ring_peer(target):
        return {"gy": target // GZ, "gz": target % GZ}

    wz_copy = pltpu.make_async_copy(wz_hbm, wz, wsem.at[0])
    wxy_copy = pltpu.make_async_copy(wxy_hbm, wxy, wsem.at[1])
    wz_copy.start()
    wxy_copy.start()

    barrier = pltpu.get_barrier_semaphore()

    @pl.loop(0, GX - 1)
    def _(i):
        pl.semaphore_signal(
            barrier, inc=1, device_id=plane_peer(plane_step(i)), device_id_type=MESH
        )

    @pl.loop(0, RING - 1)
    def _(i):
        pl.semaphore_signal(
            barrier, inc=1, device_id=ring_peer(ring_step(i)), device_id_type=MESH
        )

    coefs = dot3(halves(basis_ref[...]), halves(blocks_ref[...]), NT)
    cells = cells_ref[...].astype(F32)
    radius = (HALO - ridx_ref[...]).astype(F32)
    rate = jnp.zeros((1, 32), F32)
    for e in range(16):
        rate = rate + jnp.where(eidx_ref[...] == e, exps_ref[e], 0.0)
    rate = rate / (radius * radius)
    data = jnp.concatenate(
        [coefs, cells, offsets_ref[...], rate, radius, jnp.zeros((56, 32), F32)], 0
    )
    owner = cells_ref[0:1, :] // CX
    same_pair = iota((32, 32), 0) == iota((32, 32), 1)
    owner_column = jnp.sum(
        jnp.where(same_pair, owner.astype(F32), 0.0), axis=1, keepdims=True
    ).astype(jnp.int32)
    earlier = (owner_column == owner) & (iota((32, 32), 0) < iota((32, 32), 1))
    within = jnp.sum(jnp.where(earlier, 1.0, 0.0), axis=0, keepdims=True).astype(jnp.int32)
    base = owner * 2 + within
    row = iota((SLOTS, 1), 0)
    slot = row % 8
    code = (row // 8 + slot // 2 + (GX - 1)) % GX * 2 + slot % 2
    code = jnp.where(slot < 6, code, -1)
    pick = jnp.where(code == base, 1.0, 0.0).astype(BF16)
    high, middle = halves(data)
    rest = (data - high.astype(F32) - middle.astype(F32)).astype(BF16)
    routed = dot(pick, high, NT) + dot(pick, middle, NT) + dot(pick, rest, NT)
    out1[...] = routed.reshape(GX, 8, 128)
    recv1[gx] = out1[gx]

    pl.semaphore_wait(barrier, GX + RING - 2)

    def copy1(target, source):
        return pltpu.make_async_remote_copy(
            src_ref=out1.at[target], dst_ref=recv1.at[source],
            send_sem=s1.at[target], recv_sem=r1.at[source],
            device_id=plane_peer(target), device_id_type=MESH,
        )

    @pl.loop(0, GX - 1)
    def _(i):
        copy1(plane_step(i), gx).start()

    @pl.loop(1, GX)
    def _(d):
        other = lax.rem(gx + d, GX)
        copy1(other, other).wait_recv()

    table = recv1[...].reshape(SLOTS, 128).T
    cx, cy, cz = table[64:65], table[65:66], table[66:67]
    ox, oy, oz = table[67:68], table[68:69], table[69:70]
    rates, radii = table[70:71], table[71:72]

    def factors(offset_cells, offset_in):
        distance = offset_cells - offset_in
        inside = jnp.abs(offset_cells) <= radii
        envelope = jnp.where(inside, jnp.exp(-rates * distance * distance), 0.0)
        scaled = distance * (1.0 / HALO)
        first = envelope * scaled
        second = first * scaled
        return [envelope, first, second, second * scaled]

    step_x = (gx * CX + iota((CX, 1), 0)).astype(F32) - cx
    step_x = jnp.where(step_x > 128.0, step_x - 256.0, step_x)
    step_x = jnp.where(step_x < -128.0, step_x + 256.0, step_x)
    along_x = factors(step_x, ox)
    for j in range(4):
        for k in range(4):
            total = table[j * 4 + k : j * 4 + k + 1] * along_x[0]
            for i in range(1, 4):
                at = i * 16 + j * 4 + k
                total = total + table[at : at + 1] * along_x[i]
            amps[j * 4 + k] = total
    along_y = factors((gy * CY - HALO + iota((48, 1), 0)).astype(F32) - cy, oy)
    z_row = iota((256, 1), 0)
    rim = z_row % 16
    z_cell = jnp.where(
        z_row < CZ, z_row, jnp.where(rim < HALO, CZ + rim, rim - 2 * HALO)
    )
    along_z = factors((gz * CZ + z_cell).astype(F32) - cz, oz)

    for x in range(CX):
        for k in range(4):
            total = amps[k, x : x + 1, :] * along_y[0]
            for j in range(1, 4):
                total = total + amps[j * 4 + k, x : x + 1, :] * along_y[j]
            high, low = halves(total)
            t_hi[x * 48 : (x + 1) * 48, k * SLOTS : (k + 1) * SLOTS] = high
            t_lo[x * 48 : (x + 1) * 48, k * SLOTS : (k + 1) * SLOTS] = low
    z_all = halves(jnp.concatenate(along_z, 1))
    block = dot3((t_hi[...], t_lo[...]), z_all, NT)
    keep = iota((8, 128), 1) // 16 == iota((8, 128), 0)
    for x in range(CX):
        for g in range(GROUPS):
            at = x * 48 + g * 8
            slabs[g, x * 8 : (x + 1) * 8, :] = block[at : at + 8, :128]
            slabs[g, 64 + x : 65 + x, :] = jnp.sum(
                jnp.where(keep, block[at : at + 8, 128:], 0.0), axis=0, keepdims=True
            )

    def copy3(group, source):
        return pltpu.make_async_remote_copy(
            src_ref=slabs.at[group], dst_ref=main_in.at[source],
            send_sem=s3.at[group], recv_sem=r3.at[source],
            device_id={"gz": group - 1}, device_id_type=MESH,
        )

    def copy3_rim(group, source, row_to, depth_to):
        return pltpu.make_async_remote_copy(
            src_ref=slabs.at[group], dst_ref=rim_in.at[source],
            send_sem=s3.at[group], recv_sem=r3x.at[source],
            device_id={"gy": row_to, "gz": depth_to}, device_id_type=MESH,
        )

    before, after = lax.rem(gy + GY - 1, GY), lax.rem(gy + 1, GY)

    copy3(3 - 2 * half + core, gz).start()
    copy3(4 - 2 * half - core, gz).start()
    copy3_rim(0, gz, before, GZ - 1).start()
    copy3_rim(5, gz, after, 0).start()
    copy3(2 + 2 * half - core, gz).start()
    main_in[gz] = slabs[1 + gz]

    edge = (gz == 0) | (gz == GZ - 1)

    @pl.when(jnp.logical_not(edge))
    def _():
        rim_in[...] = jnp.zeros((GZ, SLAB, 128), F32)

    wz_copy.wait()
    wxy_copy.wait()

    @pl.loop(1, GZ)
    def _(d):
        other = lax.rem(gz + d, GZ)
        copy3(1 + other, other).wait_recv()

    @pl.when(edge)
    def _():
        @pl.loop(0, GZ)
        def _(source):
            copy3_rim(0, source, before, GZ - 1).wait_recv()

    row_lane = iota((64, 128), 1)
    keep_rows = row_lane // 16 == iota((64, 128), 0) % 8
    rims = []
    for q in range(GZ):
        packed = main_in[q, 64:SLAB, :] + rim_in[q, 64:SLAB, :]
        spread = jnp.concatenate(
            [jnp.broadcast_to(packed[x : x + 1], (8, 128)) for x in range(CX)], 0
        )
        spread = jnp.where(keep_rows, spread, 0.0)
        for shift in (16, 32, 64):
            spread = spread + pltpu.roll(spread, shift, 1)
        rims.append(spread)
    for q in range(GZ):
        lines[q] = (
            main_in[q, 0:64, :]
            + rim_in[q, 0:64, :]
            + jnp.where(row_lane >= CZ - HALO, rims[(q + 1) % GZ], 0.0)
            + jnp.where(row_lane < HALO, rims[(q + GZ - 1) % GZ], 0.0)
        )
    line_parts = halves(jnp.concatenate([lines[q] for q in range(GZ)], 1))
    for c in range(8):
        columns = slice(c * 128, (c + 1) * 128)
        part = dot3(line_parts, (wz[0, :, columns], wz[1, :, columns]), NN)
        part = swap_lanes(part.reshape(8, 8, 128), 8, 1)
        first = c % 4 * 8
        out4[first : first + 8, c // 4] = part

    def copy4(target, source):
        return pltpu.make_async_remote_copy(
            src_ref=out4.at[target], dst_ref=in4.at[:, pl.ds(pl.multiple_of(source * 8, 8), 8), :],
            send_sem=s4.at[target], recv_sem=r4.at[source],
            device_id=ring_peer(target), device_id_type=MESH,
        )

    @pl.loop(0, RING - 1)
    def _(i):
        copy4(ring_step(i), me).start()

    def copy_d(target, source):
        return pltpu.make_async_remote_copy(
            src_ref=lines.at[target], dst_ref=dens_in.at[source],
            send_sem=sd.at[target], recv_sem=rd.at[source],
            device_id={"gz": target}, device_id_type=MESH,
        )

    in4[:, pl.ds(pl.multiple_of(me * 8, 8), 8), :] = out4[me]
    dens_in[gz] = lines[gz]

    @pl.loop(1, RING)
    def _(d):
        other = lax.rem(me + d, RING)
        copy4(other, other).wait_recv()

    cosines = (wxy[0], wxy[1])
    sines = (wxy[2], wxy[3])
    rows_in = halves(jnp.concatenate([in4[0], in4[1]], 1))
    with_cos = dot3(cosines, rows_in, NN)
    with_sin = dot3(sines, rows_in, NN)
    out5[0] = with_cos[:, :128] + with_sin[:, 128:]
    out5[1] = with_cos[:, 128:] - with_sin[:, :128]

    def copy5(target, source):
        return pltpu.make_async_remote_copy(
            src_ref=out5.at[:, pl.ds(pl.multiple_of(target * 8, 8), 8), :], dst_ref=in5.at[source],
            send_sem=s5.at[target], recv_sem=r5.at[source],
            device_id=plane_peer(target), device_id_type=MESH,
        )

    @pl.loop(0, GX - 1)
    def _(i):
        copy5(plane_step(i), gx).start()

    @pl.loop(1, GZ)
    def _(d):
        copy_d(lax.rem(gz + d, GZ), gz).start()

    in5[gx] = out5[:, pl.ds(pl.multiple_of(gx * 8, 8), 8), :]

    @pl.loop(1, GX)
    def _(d):
        other = lax.rem(gx + d, GX)
        copy5(other, other).wait_recv()

    sides = []
    for part in range(2):
        pieces = [
            swap_lanes(in5[h * 16 : (h + 1) * 16, part], 16, 8).reshape(128, 128)
            for h in range(2)
        ]
        sides.append(jnp.concatenate(pieces, 1))
    x_lines = halves(jnp.concatenate(sides, 0))
    with_cos = dot3(x_lines, cosines, NN)
    with_sin = dot3(x_lines, sines, NN)
    spec_ref[0] = (with_cos[:128] + with_sin[128:]).reshape(16, 8, NXY)
    spec_ref[1] = (with_cos[128:] - with_sin[:128]).reshape(16, 8, NXY)

    @pl.loop(1, GZ)
    def _(d):
        other = lax.rem(gz + d, GZ)
        copy_d(other, other).wait_recv()

    for q in range(GZ):
        dens_ref[:, q * 8 : (q + 1) * 8, :] = dens_in[q].reshape(8, 8, 128)

    @pl.loop(1, GX)
    def _(d):
        other = lax.rem(gx + d, GX)
        copy1(other, gx).wait_send()
        copy5(other, gx).wait_send()

    @pl.loop(1, RING)
    def _(d):
        copy4(lax.rem(me + d, RING), me).wait_send()

    @pl.loop(1, GZ)
    def _(d):
        other = lax.rem(gz + d, GZ)
        copy3(1 + other, gz).wait_send()
        copy_d(other, gz).wait_send()

    copy3_rim(0, gz, before, GZ - 1).wait_send()
    copy3_rim(5, gz, after, 0).wait_send()


def solution(mesh):
    wz = np.stack(np_halves(depth_matrix()))
    cos_m, sin_m = plane_matrices()
    wxy = np.stack([*np_halves(cos_m), *np_halves(sin_m)])
    vmem = pl.BlockSpec(memory_space=pltpu.VMEM)
    anywhere = pl.BlockSpec(memory_space=pl.ANY)
    dma = pltpu.SemaphoreType.DMA
    call = pl.pallas_call(
        kernel,
        out_shape=(
            jax.ShapeDtypeStruct((CX, CY, CZ), F32),
            jax.ShapeDtypeStruct((2, 16, 8, NXY), F32),
        ),
        in_specs=[vmem] * 6 + [pl.BlockSpec(memory_space=pltpu.SMEM), anywhere, anywhere],
        out_specs=(vmem, vmem),
        scratch_shapes=[
            pltpu.VMEM((2, NZ, 2 * NZ), BF16),
            pltpu.VMEM((4, NXY, NXY), BF16),
            pltpu.VMEM((GX, 8, 128), F32),
            pltpu.VMEM((GX, 8, 128), F32),
            pltpu.VMEM((16, 8, SLOTS), F32),
            pltpu.VMEM((384, 4 * SLOTS), BF16),
            pltpu.VMEM((384, 4 * SLOTS), BF16),
            pltpu.VMEM((GROUPS, SLAB, 128), F32),
            pltpu.VMEM((GZ, SLAB, 128), F32),
            pltpu.VMEM((GZ, SLAB, 128), F32),
            pltpu.VMEM((GZ, 64, 128), F32),
            pltpu.VMEM((RING, 2, 8, 128), F32),
            pltpu.VMEM((2, NXY, 128), F32),
            pltpu.VMEM((2, NXY, 128), F32),
            pltpu.VMEM((GX, 2, 8, 128), F32),
            pltpu.VMEM((GZ, 64, 128), F32),
            dma((2,)),
            dma((GX,)), dma((GX,)),
            dma((GROUPS,)), dma((GZ,)), dma((GZ,)),
            dma((RING,)), dma((RING,)),
            dma((GX,)), dma((GX,)),
            dma((GZ,)), dma((GZ,)),
        ],
        compiler_params=pltpu.CompilerParams(collective_id=0, has_side_effects=True),
        name="pair_grid_transform",
    )

    def shards(blocks, basis, cells, offsets, eidx, ridx, exps):
        return call(
            blocks.T, basis.T, cells, offsets, eidx.reshape(1, -1), ridx.reshape(1, -1), exps,
            jnp.asarray(wz), jnp.asarray(wxy),
        )

    split = ("gx", "gy", "gz")
    placed = (P(None, split), P(), P(None, split), P(None, split), P(split), P(split), P())
    return jax.shard_map(
        shards,
        mesh=mesh,
        in_specs=placed,
        out_specs=(P("gx", "gy", "gz"), P(None, ("gy", "gz"), "gx", None)),
        check_vma=False,
    )
```

```python
import math

import jax
import jax.numpy as jnp
import ml_dtypes
import numpy as np
from jax import lax
from jax.experimental import pallas as pl
from jax.experimental.pallas import tpu as pltpu
from jax.sharding import PartitionSpec as P

HALO = 8
CX, CY, CZ = 8, 32, 128
GX, GY, GZ = 32, 8, 4
RING = GY * GZ
NZ = GZ * CZ
NXY = 256
SLOTS = GX * 8
GROUPS = 6
SLAB = 36
HX = 4
MESH = pl.DeviceIdType.MESH
F32 = jnp.float32
BF16 = jnp.bfloat16

NN = (((1,), (0,)), ((), ()))
NT = (((1,), (1,)), ((), ()))


def halves(value):
    high = value.astype(BF16)
    return high, (value - high.astype(F32)).astype(BF16)


def dot(a, b, dims):
    return lax.dot_general(a, b, dims, preferred_element_type=F32)


def dot3(a, b, dims):
    rows = a[0].shape[0]
    both = dot(jnp.concatenate(a, 0), b[0], dims)
    return both[:rows] + (both[rows:] + dot(a[0], b[1], dims))


def unrolled(count):
    def run(body):
        for i in range(count):
            body(i)

    return run


def np_halves(value):
    value = value.astype(np.float32)
    high = value.astype(ml_dtypes.bfloat16)
    return high, (value - high.astype(np.float32)).astype(ml_dtypes.bfloat16)


def depth_matrix():
    lane = np.arange(128)
    kz = 16 * (8 * np.arange(4)[:, None] + lane[None, :] % 8) + lane[None, :] // 8
    phase = np.arange(NZ)[:, None] * kz.reshape(-1)[None, :] % NZ
    angle = phase * (2.0 * math.pi / NZ)
    scale = 1.0 / math.sqrt(NZ)
    return np.concatenate([np.cos(angle) * scale, -np.sin(angle) * scale], 1)


def plane_matrices():
    index = np.arange(NXY)
    angle = (index[:, None] * index[None, :] % NXY) * (2.0 * math.pi / NXY)
    scale = 1.0 / math.sqrt(NXY)
    order = np.arange(NXY).reshape(GX, 2, HX).transpose(1, 0, 2).reshape(-1)
    cosine, sine = np.cos(angle) * scale, np.sin(angle) * scale
    return cosine, sine, cosine[order], sine[order]


def iota(shape, axis):
    return lax.broadcasted_iota(jnp.int32, shape, axis)


def swap_lanes(v, count, group):
    bit = 1
    while bit < count:
        shift = bit * group
        v = v.reshape(count // (2 * bit), 2, bit * 8, 128)
        a = v[:, 0].reshape(count * 4, 128)
        c = v[:, 1].reshape(count * 4, 128)
        low = (iota((count * 4, 128), 1) // shift) % 2 == 0
        na = jnp.where(low, a, pltpu.roll(c, shift, 1))
        nc = jnp.where(low, pltpu.roll(a, 128 - shift, 1), c)
        parts = (count // (2 * bit), 1, bit * 8, 128)
        v = jnp.concatenate([na.reshape(parts), nc.reshape(parts)], 1)
        v = v.reshape(count, 8, 128)
        bit *= 2
    return v


def kernel(
    blocks_ref, basis_ref, cells_ref, offsets_ref, eidx_ref, ridx_ref, exps_ref,
    wz_hbm, wxy_hbm, dens_ref, spec_ref,
    wz, wxy, out1, recv1, amps, t_hi, t_lo, slabs, main_in, rim_in, lines,
    out4, in4, out5, in5, dens_in,
    wsem, s1, r1, s3, r3, r3x, s4, r4, s5, r5, sd, rd,
):
    gx, gy, gz = lax.axis_index("gx"), lax.axis_index("gy"), lax.axis_index("gz")
    me = gy * GZ + gz

    half, core = gz >> 1, gz & 1

    def far_first(i, reach):
        return (reach - (i + 1) // 2) * (2 * (i % 2) - 1)

    def plane_step(i):
        row = ((gx >> 2) + far_first(i // 4, 4)) & 7
        return row * 4 + (((gx & 3) + far_first(i % 4, 2)) & 3)

    def ring_step(i):
        depth = (gy + 8 * half + far_first(i // 2, 8)) & 15
        return (depth & 7) * GZ + (depth >> 3) * 2 + ((core + 1 + i) & 1)

    def arrived(ref, semaphore):
        pltpu.make_async_copy(ref, ref, semaphore).wait()

    def plane_peer(target):
        return {"gx": target}

    def ring_peer(target):
        return {"gy": target >> 2, "gz": target & 3}

    wz_copy = pltpu.make_async_copy(wz_hbm, wz, wsem.at[0])
    wxy_copy = pltpu.make_async_copy(wxy_hbm, wxy, wsem.at[1])
    wz_copy.start()
    wxy_copy.start()

    barrier = pltpu.get_barrier_semaphore()

    @unrolled(GX - 1)
    def _(i):
        pl.semaphore_signal(
            barrier, inc=1, device_id=plane_peer(plane_step(i)), device_id_type=MESH
        )

    @unrolled(RING - 1)
    def _(i):
        pl.semaphore_signal(
            barrier, inc=1, device_id=ring_peer(ring_step(i)), device_id_type=MESH
        )

    coefs = dot3(halves(basis_ref[...]), halves(blocks_ref[...]), NT)
    cells = cells_ref[...].astype(F32)
    radius = (HALO - ridx_ref[...]).astype(F32)
    rate = jnp.zeros((1, 32), F32)
    for e in range(16):
        rate = rate + jnp.where(eidx_ref[...] == e, exps_ref[e], 0.0)
    rate = rate / (radius * radius)
    data = jnp.concatenate(
        [coefs, cells, offsets_ref[...], rate, radius, jnp.zeros((56, 32), F32)], 0
    )
    owner = cells_ref[0:1, :] // CX
    same_pair = iota((32, 32), 0) == iota((32, 32), 1)
    owner_column = jnp.sum(
        jnp.where(same_pair, owner.astype(F32), 0.0), axis=1, keepdims=True
    ).astype(jnp.int32)
    earlier = (owner_column == owner) & (iota((32, 32), 0) < iota((32, 32), 1))
    within = jnp.sum(jnp.where(earlier, 1.0, 0.0), axis=0, keepdims=True).astype(jnp.int32)
    base = owner * 2 + within
    row = iota((SLOTS, 1), 0)
    slot = row % 8
    code = (row // 8 + slot // 2 + (GX - 1)) % GX * 2 + slot % 2
    code = jnp.where(slot < 6, code, -1)
    pick = jnp.where(code == base, 1.0, 0.0).astype(BF16)
    high, middle = halves(data)
    rest = (data - high.astype(F32) - middle.astype(F32)).astype(BF16)
    routed = dot(pick, high, NT) + dot(pick, middle, NT) + dot(pick, rest, NT)
    out1[...] = routed.reshape(GX, 8, 128)
    recv1[gx] = out1[gx]

    pl.semaphore_wait(barrier, GX + RING - 2)

    def copy1(target, source):
        return pltpu.make_async_remote_copy(
            src_ref=out1.at[target], dst_ref=recv1.at[source],
            send_sem=s1, recv_sem=r1,
            device_id=plane_peer(target), device_id_type=MESH,
        )

    @unrolled(GX - 1)
    def _(i):
        copy1(plane_step(i), gx).start()

    arrived(recv1.at[0 : GX - 1], r1)

    table = recv1[...].reshape(SLOTS, 128).T
    cx, cy, cz = table[64:65], table[65:66], table[66:67]
    ox, oy, oz = table[67:68], table[68:69], table[69:70]
    rates, radii = table[70:71], table[71:72]

    def factors(offset_cells, offset_in):
        distance = offset_cells - offset_in
        inside = jnp.abs(offset_cells) <= radii
        envelope = jnp.where(inside, jnp.exp(-rates * distance * distance), 0.0)
        scaled = distance * (1.0 / HALO)
        first = envelope * scaled
        second = first * scaled
        return [envelope, first, second, second * scaled]

    step_x = (gx * CX + iota((CX, 1), 0)).astype(F32) - cx
    step_x = jnp.where(step_x > 128.0, step_x - 256.0, step_x)
    step_x = jnp.where(step_x < -128.0, step_x + 256.0, step_x)
    along_x = factors(step_x, ox)
    for j in range(4):
        for k in range(4):
            total = table[j * 4 + k : j * 4 + k + 1] * along_x[0]
            for i in range(1, 4):
                at = i * 16 + j * 4 + k
                total = total + table[at : at + 1] * along_x[i]
            amps[j * 4 + k] = total
    along_y = factors((gy * CY - HALO + iota((48, 1), 0)).astype(F32) - cy, oy)
    z_row = iota((256, 1), 0)
    rim = z_row % 16
    z_cell = jnp.where(
        z_row < CZ, z_row, jnp.where(rim < HALO, CZ + rim, rim - 2 * HALO)
    )
    along_z = factors((gz * CZ + z_cell).astype(F32) - cz, oz)

    z_all = halves(jnp.concatenate(along_z, 1))
    keep = iota((8, 128), 1) // 16 == iota((8, 128), 0)

    def copy3(h, group, source):
        return pltpu.make_async_remote_copy(
            src_ref=slabs.at[h, group], dst_ref=main_in.at[h, source],
            send_sem=s3.at[h], recv_sem=r3.at[h],
            device_id={"gz": group - 1}, device_id_type=MESH,
        )

    def copy3_rim(h, group, source, row_to, depth_to):
        return pltpu.make_async_remote_copy(
            src_ref=slabs.at[h, group], dst_ref=rim_in.at[h, source],
            send_sem=s3.at[h], recv_sem=r3x.at[h],
            device_id={"gy": row_to, "gz": depth_to}, device_id_type=MESH,
        )

    before, after = lax.rem(gy + GY - 1, GY), lax.rem(gy + 1, GY)

    for h in range(2):
        for x in range(HX):
            for k in range(4):
                at = h * HX + x
                total = amps[k, at : at + 1, :] * along_y[0]
                for j in range(1, 4):
                    total = total + amps[j * 4 + k, at : at + 1, :] * along_y[j]
                high, low = halves(total)
                t_hi[x * 48 : (x + 1) * 48, k * SLOTS : (k + 1) * SLOTS] = high
                t_lo[x * 48 : (x + 1) * 48, k * SLOTS : (k + 1) * SLOTS] = low
        block = dot3((t_hi[...], t_lo[...]), z_all, NT)
        for x in range(HX):
            for g in range(GROUPS):
                at = x * 48 + g * 8
                slabs[h, g, x * 8 : (x + 1) * 8, :] = block[at : at + 8, :128]
                slabs[h, g, 32 + x : 33 + x, :] = jnp.sum(
                    jnp.where(keep, block[at : at + 8, 128:], 0.0), axis=0, keepdims=True
                )
        copy3(h, 3 - 2 * half + core, gz).start()
        copy3(h, 4 - 2 * half - core, gz).start()
        copy3_rim(h, 0, gz, before, GZ - 1).start()
        copy3_rim(h, 5, gz, after, 0).start()
        copy3(h, 2 + 2 * half - core, gz).start()
        main_in[h, gz] = slabs[h, 1 + gz]

    edge = (gz == 0) | (gz == GZ - 1)

    @pl.when(jnp.logical_not(edge))
    def _():
        rim_in[...] = jnp.zeros((2, GZ, SLAB, 128), F32)

    wz_copy.wait()
    wxy_copy.wait()

    def copy4(h, target, source):
        return pltpu.make_async_remote_copy(
            src_ref=out4.at[h, target],
            dst_ref=in4.at[h, pl.ds(pl.multiple_of(source * 8, 8), 8), :],
            send_sem=s4.at[h], recv_sem=r4.at[h],
            device_id=ring_peer(target), device_id_type=MESH,
        )

    def copy5(h, target, source):
        return pltpu.make_async_remote_copy(
            src_ref=out5.at[h, pl.ds(pl.multiple_of(target * 8, 8), 8), :],
            dst_ref=in5.at[h, source],
            send_sem=s5.at[h], recv_sem=r5.at[h],
            device_id=plane_peer(target), device_id_type=MESH,
        )

    def copy_d(target, source):
        return pltpu.make_async_remote_copy(
            src_ref=lines.at[target], dst_ref=dens_in.at[source],
            send_sem=sd, recv_sem=rd,
            device_id={"gz": target}, device_id_type=MESH,
        )

    row_lane = iota((32, 128), 1)
    keep_rows = row_lane // 16 == iota((32, 128), 0) % 8
    for h in range(2):
        arrived(main_in.at[h, 0 : GZ - 1], r3.at[h])

        @pl.when(edge)
        def _():
            arrived(rim_in.at[h], r3x.at[h])

        rims = []
        for q in range(GZ):
            packed = main_in[h, q, 32:SLAB, :] + rim_in[h, q, 32:SLAB, :]
            spread = jnp.concatenate(
                [jnp.broadcast_to(packed[x : x + 1], (8, 128)) for x in range(HX)], 0
            )
            spread = jnp.where(keep_rows, spread, 0.0)
            for shift in (16, 32, 64):
                spread = spread + pltpu.roll(spread, shift, 1)
            rims.append(spread)
        for q in range(GZ):
            lines[q, h * 32 : (h + 1) * 32, :] = (
                main_in[h, q, 0:32, :]
                + rim_in[h, q, 0:32, :]
                + jnp.where(row_lane >= CZ - HALO, rims[(q + 1) % GZ], 0.0)
                + jnp.where(row_lane < HALO, rims[(q + GZ - 1) % GZ], 0.0)
            )
        line_parts = halves(
            jnp.concatenate([lines[q, h * 32 : (h + 1) * 32, :] for q in range(GZ)], 1)
        )
        lines_hat = dot3(line_parts, (wz[0], wz[1]), NN)
        for c in range(4):
            pair = [lines_hat[:, p * 512 + c * 128 : p * 512 + (c + 1) * 128] for p in range(2)]
            part = jnp.concatenate([v.reshape(HX, 8, 128) for v in pair], 0)
            out4[h, c * 8 : (c + 1) * 8] = swap_lanes(part, 8, 1)

        @unrolled(RING - 1)
        def _(i):
            copy4(h, ring_step(i), me).start()

        in4[h, pl.ds(pl.multiple_of(me * 8, 8), 8), :] = out4[h, me]

    dens_in[gz] = lines[gz]

    cosines = (wxy[0], wxy[1])
    sines = (wxy[2], wxy[3])
    real_lane = iota((NXY, 128), 1) // HX % 2 == 0
    for h in range(2):
        arrived(in4.at[h, 0 : NXY - 8], r4.at[h])

        rows_in = halves(in4[h])
        with_cos = dot3(cosines, rows_in, NN)
        with_sin = dot3(sines, rows_in, NN)
        out5[h] = with_cos + jnp.where(
            real_lane, pltpu.roll(with_sin, 128 - HX, 1), -pltpu.roll(with_sin, HX, 1)
        )

        @unrolled(GX - 1)
        def _(i):
            copy5(h, plane_step(i), gx).start()

        in5[h, gx] = out5[h, pl.ds(pl.multiple_of(gx * 8, 8), 8), :]

    @pl.loop(1, GZ)
    def _(d):
        copy_d(lax.rem(gz + d, GZ), gz).start()

    with_cos = with_sin = None
    for h in range(2):
        arrived(in5.at[h, 0 : GX - 1], r5.at[h])

        x_lines = swap_lanes(in5[h], 32, HX).reshape(16, 2, 8, 128)
        x_lines = jnp.concatenate(
            [x_lines[:, p].reshape(128, 128) for p in range(2)], 0
        )
        x_lines = halves(x_lines)
        rows = slice(h * 128, (h + 1) * 128)
        add_cos = dot3(x_lines, (wxy[4, rows], wxy[5, rows]), NN)
        add_sin = dot3(x_lines, (wxy[6, rows], wxy[7, rows]), NN)
        with_cos = add_cos if h == 0 else with_cos + add_cos
        with_sin = add_sin if h == 0 else with_sin + add_sin
    spec_ref[0] = (with_cos[:128] + with_sin[128:]).reshape(16, 8, NXY)
    spec_ref[1] = (with_cos[128:] - with_sin[:128]).reshape(16, 8, NXY)

    arrived(dens_in.at[0 : GZ - 1], rd)
    for q in range(GZ):
        dens_ref[:, q * 8 : (q + 1) * 8, :] = dens_in[q].reshape(8, 8, 128)

    arrived(out1.at[0 : GX - 1], s1)
    arrived(lines.at[0 : GZ - 1], sd)
    for h in range(2):
        arrived(out5.at[h, 0 : NXY - 8], s5.at[h])
        arrived(out4.at[h, 0 : RING - 1], s4.at[h])
        arrived(slabs.at[h, 0 : GROUPS - 1], s3.at[h])


def solution(mesh):
    wz = np.stack(np_halves(depth_matrix()))
    wxy = np.concatenate([np.stack(np_halves(m)) for m in plane_matrices()])
    vmem = pl.BlockSpec(memory_space=pltpu.VMEM)
    anywhere = pl.BlockSpec(memory_space=pl.ANY)
    dma = pltpu.SemaphoreType.DMA
    call = pl.pallas_call(
        kernel,
        out_shape=(
            jax.ShapeDtypeStruct((CX, CY, CZ), F32),
            jax.ShapeDtypeStruct((2, 16, 8, NXY), F32),
        ),
        in_specs=[vmem] * 6 + [pl.BlockSpec(memory_space=pltpu.SMEM), anywhere, anywhere],
        out_specs=(vmem, vmem),
        scratch_shapes=[
            pltpu.VMEM((2, NZ, 2 * NZ), BF16),
            pltpu.VMEM((8, NXY, NXY), BF16),
            pltpu.VMEM((GX, 8, 128), F32),
            pltpu.VMEM((GX, 8, 128), F32),
            pltpu.VMEM((16, 8, SLOTS), F32),
            pltpu.VMEM((192, 4 * SLOTS), BF16),
            pltpu.VMEM((192, 4 * SLOTS), BF16),
            pltpu.VMEM((2, GROUPS, SLAB, 128), F32),
            pltpu.VMEM((2, GZ, SLAB, 128), F32),
            pltpu.VMEM((2, GZ, SLAB, 128), F32),
            pltpu.VMEM((GZ, 64, 128), F32),
            pltpu.VMEM((2, RING, 8, 128), F32),
            pltpu.VMEM((2, NXY, 128), F32),
            pltpu.VMEM((2, NXY, 128), F32),
            pltpu.VMEM((2, GX, 8, 128), F32),
            pltpu.VMEM((GZ, 64, 128), F32),
            dma((2,)),
            dma, dma,
            dma((2,)), dma((2,)), dma((2,)),
            dma((2,)), dma((2,)),
            dma((2,)), dma((2,)),
            dma, dma,
        ],
        compiler_params=pltpu.CompilerParams(collective_id=0, has_side_effects=True),
        name="pair_grid_transform",
    )

    def shards(blocks, basis, cells, offsets, eidx, ridx, exps):
        return call(
            blocks.T, basis.T, cells, offsets, eidx.reshape(1, -1), ridx.reshape(1, -1), exps,
            jnp.asarray(wz), jnp.asarray(wxy),
        )

    split = ("gx", "gy", "gz")
    placed = (P(None, split), P(), P(None, split), P(None, split), P(split), P(split), P())
    return jax.shard_map(
        shards,
        mesh=mesh,
        in_specs=placed,
        out_specs=(P("gx", "gy", "gz"), P(None, ("gy", "gz"), "gx", None)),
        check_vma=False,
    )
```

```python
import math

import jax
import jax.numpy as jnp
import ml_dtypes
import numpy as np
from jax import lax
from jax.experimental import pallas as pl
from jax.experimental.pallas import tpu as pltpu
from jax.sharding import PartitionSpec as P

HALO = 8
CX, CY, CZ = 8, 32, 128
GX, GY, GZ = 32, 8, 4
RING = GY * GZ
NZ = GZ * CZ
NXY = 256
SLOTS = GX * 8
GROUPS = 6
SLAB = 36
HX = 4
NPOLY = 64
MESH = pl.DeviceIdType.MESH
F32 = jnp.float32
BF16 = jnp.bfloat16

NN = (((1,), (0,)), ((), ()))
NT = (((1,), (1,)), ((), ()))


def halves(value):
    high = value.astype(BF16)
    return high, (value - high.astype(F32)).astype(BF16)


def dot(a, b, dims):
    return lax.dot_general(a, b, dims, preferred_element_type=F32)


def dot3(a, b, dims):
    rows = a[0].shape[0]
    both = dot(jnp.concatenate(a, 0), b[0], dims)
    return both[:rows] + (both[rows:] + dot(a[0], b[1], dims))


def unrolled(count):
    def run(body):
        for i in range(count):
            body(i)

    return run


def np_halves(value):
    value = value.astype(np.float32)
    high = value.astype(ml_dtypes.bfloat16)
    return high, (value - high.astype(np.float32)).astype(ml_dtypes.bfloat16)


def depth_matrix():
    lane = np.arange(128)
    kz = 16 * (8 * np.arange(4)[:, None] + lane[None, :] % 8) + lane[None, :] // 8
    phase = np.arange(NZ)[:, None] * kz.reshape(-1)[None, :] % NZ
    angle = phase * (2.0 * math.pi / NZ)
    scale = 1.0 / math.sqrt(NZ)
    return np.concatenate([np.cos(angle) * scale, -np.sin(angle) * scale], 1)


def plane_matrices():
    index = np.arange(NXY)
    angle = (index[:, None] * index[None, :] % NXY) * (2.0 * math.pi / NXY)
    scale = 1.0 / math.sqrt(NXY)
    order = np.arange(NXY).reshape(GX, 2, HX).transpose(1, 0, 2).reshape(-1)
    cosine, sine = np.cos(angle) * scale, np.sin(angle) * scale
    return cosine, sine, cosine[order], sine[order]


def iota(shape, axis):
    return lax.broadcasted_iota(jnp.int32, shape, axis)


def swap_lanes(v, count, group):
    bit = 1
    while bit < count:
        shift = bit * group
        v = v.reshape(count // (2 * bit), 2, bit * 8, 128)
        a = v[:, 0].reshape(count * 4, 128)
        c = v[:, 1].reshape(count * 4, 128)
        low = (iota((count * 4, 128), 1) // shift) % 2 == 0
        na = jnp.where(low, a, pltpu.roll(c, shift, 1))
        nc = jnp.where(low, pltpu.roll(a, 128 - shift, 1), c)
        parts = (count // (2 * bit), 1, bit * 8, 128)
        v = jnp.concatenate([na.reshape(parts), nc.reshape(parts)], 1)
        v = v.reshape(count, 8, 128)
        bit *= 2
    return v


def kernel(
    blocks_hbm, basis_hbm, cells_hbm, offsets_hbm, eidx_hbm, ridx_hbm, exps_ref,
    wz_hbm, wxy_hbm, dens_in, in5,
    blocks_ref, basis_ref, cells_ref, offsets_ref, eidx_ref, ridx_ref,
    wz, wxy, out1, recv1, amps, t_hi, t_lo, slabs, main_in, rim_in, lines,
    out4, in4, out5,
    wsem, s1, r1, s3, r3, r3x, s4, r4, s5, r5, sd, rd,
):
    gx, gy, gz = lax.axis_index("gx"), lax.axis_index("gy"), lax.axis_index("gz")
    me = gy * GZ + gz

    half, core = gz >> 1, gz & 1

    def far_first(i, reach):
        return (reach - (i + 1) // 2) * (2 * (i % 2) - 1)

    def plane_step(i):
        row = ((gx >> 2) + far_first(i // 4, 4)) & 7
        return row * 4 + (((gx & 3) + far_first(i % 4, 2)) & 3)

    def ring_step(i):
        depth = (gy + 8 * half + far_first(i // 2, 8)) & 15
        return (depth & 7) * GZ + (depth >> 3) * 2 + ((core + 1 + i) & 1)

    def arrived(ref, semaphore):
        pltpu.make_async_copy(ref, ref, semaphore).wait()

    def plane_peer(target):
        return {"gx": target}

    def ring_peer(target):
        return {"gy": target >> 2, "gz": target & 3}

    loads = [
        pltpu.make_async_copy(source, target, wsem.at[2 + n])
        for n, (source, target) in enumerate((
            (blocks_hbm, blocks_ref), (basis_hbm, basis_ref), (cells_hbm, cells_ref),
            (offsets_hbm, offsets_ref), (eidx_hbm, eidx_ref), (ridx_hbm, ridx_ref),
        ))
    ]
    for load in loads:
        load.start()
    wz_copy = pltpu.make_async_copy(wz_hbm, wz, wsem.at[0])
    wxy_copy = pltpu.make_async_copy(wxy_hbm, wxy, wsem.at[1])
    wz_copy.start()
    wxy_copy.start()

    barrier = pltpu.get_barrier_semaphore()

    @unrolled(GX - 1)
    def _(i):
        pl.semaphore_signal(
            barrier, inc=1, device_id=plane_peer(plane_step(i)), device_id_type=MESH
        )

    @unrolled(RING - 1)
    def _(i):
        pl.semaphore_signal(
            barrier, inc=1, device_id=ring_peer(ring_step(i)), device_id_type=MESH
        )

    for load in loads:
        load.wait()
    coefs = dot3(halves(basis_ref[...]), halves(blocks_ref[...]), NT)
    cells = cells_ref[...].astype(F32)
    radius = (HALO - ridx_ref[...]).astype(F32)
    rate = jnp.zeros((1, 32), F32)
    for e in range(16):
        rate = rate + jnp.where(eidx_ref[...] == e, exps_ref[e], 0.0)
    rate = rate / (radius * radius)
    data = jnp.concatenate(
        [coefs, cells, offsets_ref[...], rate, radius, jnp.zeros((56, 32), F32)], 0
    )
    owner = cells_ref[0:1, :] // CX
    same_pair = iota((32, 32), 0) == iota((32, 32), 1)
    owner_column = jnp.sum(
        jnp.where(same_pair, owner.astype(F32), 0.0), axis=1, keepdims=True
    ).astype(jnp.int32)
    earlier = (owner_column == owner) & (iota((32, 32), 0) < iota((32, 32), 1))
    within = jnp.sum(jnp.where(earlier, 1.0, 0.0), axis=0, keepdims=True).astype(jnp.int32)
    base = owner * 2 + within
    row = iota((SLOTS, 1), 0)
    slot = row % 8
    code = (row // 8 + slot // 2 + (GX - 1)) % GX * 2 + slot % 2
    code = jnp.where(slot < 6, code, -1)
    pick = jnp.where(code == base, 1.0, 0.0).astype(BF16)
    high, middle = halves(data)
    rest = (data - high.astype(F32) - middle.astype(F32)).astype(BF16)
    routed = dot(pick, high, NT) + dot(pick, middle, NT) + dot(pick, rest, NT)
    out1[...] = routed.reshape(GX, 8, 128)
    recv1[gx] = out1[gx]

    pl.semaphore_wait(barrier, GX + RING - 2)

    def copy1(target, source):
        return pltpu.make_async_remote_copy(
            src_ref=out1.at[target], dst_ref=recv1.at[source],
            send_sem=s1, recv_sem=r1,
            device_id=plane_peer(target), device_id_type=MESH,
        )

    @unrolled(GX - 1)
    def _(i):
        copy1(plane_step(i), gx).start()

    arrived(recv1.at[0 : GX - 1], r1)

    table = recv1[...].reshape(SLOTS, 128).T
    cx, cy, cz = table[64:65], table[65:66], table[66:67]
    ox, oy, oz = table[67:68], table[68:69], table[69:70]
    rates, radii = table[70:71], table[71:72]

    def factors(offset_cells, offset_in):
        distance = offset_cells - offset_in
        inside = jnp.abs(offset_cells) <= radii
        envelope = jnp.where(inside, jnp.exp(-rates * distance * distance), 0.0)
        scaled = distance * (1.0 / HALO)
        first = envelope * scaled
        second = first * scaled
        return [envelope, first, second, second * scaled]

    step_x = (gx * CX + iota((CX, 1), 0)).astype(F32) - cx
    step_x = jnp.where(step_x > 128.0, step_x - 256.0, step_x)
    step_x = jnp.where(step_x < -128.0, step_x + 256.0, step_x)
    along_x = factors(step_x, ox)
    for j in range(4):
        for k in range(4):
            total = table[j * 4 + k : j * 4 + k + 1] * along_x[0]
            for i in range(1, 4):
                at = i * 16 + j * 4 + k
                total = total + table[at : at + 1] * along_x[i]
            amps[j * 4 + k] = total
    along_y = factors((gy * CY - HALO + iota((48, 1), 0)).astype(F32) - cy, oy)
    z_row = iota((256, 1), 0)
    rim = z_row % 16
    z_cell = jnp.where(
        z_row < CZ, z_row, jnp.where(rim < HALO, CZ + rim, rim - 2 * HALO)
    )
    along_z = factors((gz * CZ + z_cell).astype(F32) - cz, oz)

    z_all = halves(jnp.concatenate(along_z, 1))
    keep = iota((8, 128), 1) // 16 == iota((8, 128), 0)

    def copy3(h, group, source):
        return pltpu.make_async_remote_copy(
            src_ref=slabs.at[h, group], dst_ref=main_in.at[h, source],
            send_sem=s3.at[h], recv_sem=r3.at[h],
            device_id={"gz": group - 1}, device_id_type=MESH,
        )

    def copy3_rim(h, group, source, row_to, depth_to):
        return pltpu.make_async_remote_copy(
            src_ref=slabs.at[h, group], dst_ref=rim_in.at[h, source],
            send_sem=s3.at[h], recv_sem=r3x.at[h],
            device_id={"gy": row_to, "gz": depth_to}, device_id_type=MESH,
        )

    before, after = lax.rem(gy + GY - 1, GY), lax.rem(gy + 1, GY)

    for h in range(2):
        for x in range(HX):
            for k in range(4):
                at = h * HX + x
                total = amps[k, at : at + 1, :] * along_y[0]
                for j in range(1, 4):
                    total = total + amps[j * 4 + k, at : at + 1, :] * along_y[j]
                high, low = halves(total)
                t_hi[x * 48 : (x + 1) * 48, k * SLOTS : (k + 1) * SLOTS] = high
                t_lo[x * 48 : (x + 1) * 48, k * SLOTS : (k + 1) * SLOTS] = low
        block = dot3((t_hi[...], t_lo[...]), z_all, NT)
        for x in range(HX):
            for g in range(GROUPS):
                at = x * 48 + g * 8
                slabs[h, g, x * 8 : (x + 1) * 8, :] = block[at : at + 8, :128]
                slabs[h, g, 32 + x : 33 + x, :] = jnp.sum(
                    jnp.where(keep, block[at : at + 8, 128:], 0.0), axis=0, keepdims=True
                )
        copy3(h, 3 - 2 * half + core, gz).start()
        copy3(h, 4 - 2 * half - core, gz).start()
        copy3_rim(h, 0, gz, before, GZ - 1).start()
        copy3_rim(h, 5, gz, after, 0).start()
        copy3(h, 2 + 2 * half - core, gz).start()
        main_in[h, gz] = slabs[h, 1 + gz]

    edge = (gz == 0) | (gz == GZ - 1)

    @pl.when(jnp.logical_not(edge))
    def _():
        rim_in[...] = jnp.zeros((2, GZ, SLAB, 128), F32)

    wz_copy.wait()
    wxy_copy.wait()

    def copy4(h, target, source):
        return pltpu.make_async_remote_copy(
            src_ref=out4.at[h, target],
            dst_ref=in4.at[h, pl.ds(pl.multiple_of(source * 8, 8), 8), :],
            send_sem=s4.at[h], recv_sem=r4.at[h],
            device_id=ring_peer(target), device_id_type=MESH,
        )

    def copy5(h, target, source):
        return pltpu.make_async_remote_copy(
            src_ref=out5.at[h, pl.ds(pl.multiple_of(target * 8, 8), 8), :],
            dst_ref=in5.at[h, source],
            send_sem=s5.at[h], recv_sem=r5.at[h],
            device_id=plane_peer(target), device_id_type=MESH,
        )

    def copy_d(target, source):
        return pltpu.make_async_remote_copy(
            src_ref=lines.at[target], dst_ref=dens_in.at[source],
            send_sem=sd, recv_sem=rd,
            device_id={"gz": target}, device_id_type=MESH,
        )

    row_lane = iota((32, 128), 1)
    keep_rows = row_lane // 16 == iota((32, 128), 0) % 8
    for h in range(2):
        arrived(main_in.at[h, 0 : GZ - 1], r3.at[h])

        @pl.when(edge)
        def _():
            arrived(rim_in.at[h], r3x.at[h])

        rims = []
        for q in range(GZ):
            packed = main_in[h, q, 32:SLAB, :] + rim_in[h, q, 32:SLAB, :]
            spread = jnp.concatenate(
                [jnp.broadcast_to(packed[x : x + 1], (8, 128)) for x in range(HX)], 0
            )
            spread = jnp.where(keep_rows, spread, 0.0)
            for shift in (16, 32, 64):
                spread = spread + pltpu.roll(spread, shift, 1)
            rims.append(spread)
        for q in range(GZ):
            lines[q, h * 32 : (h + 1) * 32, :] = (
                main_in[h, q, 0:32, :]
                + rim_in[h, q, 0:32, :]
                + jnp.where(row_lane >= CZ - HALO, rims[(q + 1) % GZ], 0.0)
                + jnp.where(row_lane < HALO, rims[(q + GZ - 1) % GZ], 0.0)
            )
        line_parts = halves(
            jnp.concatenate([lines[q, h * 32 : (h + 1) * 32, :] for q in range(GZ)], 1)
        )
        lines_hat = dot3(line_parts, (wz[0], wz[1]), NN)
        for c in range(4):
            pair = [lines_hat[:, p * 512 + c * 128 : p * 512 + (c + 1) * 128] for p in range(2)]
            part = jnp.concatenate([v.reshape(HX, 8, 128) for v in pair], 0)
            out4[h, c * 8 : (c + 1) * 8] = swap_lanes(part, 8, 1)

        @unrolled(RING - 1)
        def _(i):
            copy4(h, ring_step(i), me).start()

        in4[h, pl.ds(pl.multiple_of(me * 8, 8), 8), :] = out4[h, me]

    dens_in[gz] = lines[gz]

    cosines = (wxy[0], wxy[1])
    sines = (wxy[2], wxy[3])
    real_lane = iota((NXY, 128), 1) // HX % 2 == 0
    for h in range(2):
        arrived(in4.at[h, 0 : NXY - 8], r4.at[h])

        rows_in = halves(in4[h])
        with_cos = dot3(cosines, rows_in, NN)
        with_sin = dot3(sines, rows_in, NN)
        out5[h] = with_cos + jnp.where(
            real_lane, pltpu.roll(with_sin, 128 - HX, 1), -pltpu.roll(with_sin, HX, 1)
        )

        @unrolled(GX - 1)
        def _(i):
            copy5(h, plane_step(i), gx).start()

        in5[h, gx] = out5[h, pl.ds(pl.multiple_of(gx * 8, 8), 8), :]

    @pl.loop(1, GZ)
    def _(d):
        copy_d(lax.rem(gz + d, GZ), gz).start()

    for h in range(2):
        arrived(in5.at[h, 0 : GX - 1], r5.at[h])
    arrived(dens_in.at[0 : GZ - 1], rd)
    arrived(out1.at[0 : GX - 1], s1)
    arrived(lines.at[0 : GZ - 1], sd)
    for h in range(2):
        arrived(out5.at[h, 0 : NXY - 8], s5.at[h])
        arrived(out4.at[h, 0 : RING - 1], s4.at[h])
        arrived(slabs.at[h, 0 : GROUPS - 1], s3.at[h])


def last_kernel(dens_in, in5, wx, dens_ref, spec_ref):
    with_cos = with_sin = None
    for h in range(2):
        x_lines = swap_lanes(in5[h], 32, HX).reshape(16, 2, 8, 128)
        x_lines = jnp.concatenate(
            [x_lines[:, p].reshape(128, 128) for p in range(2)], 0
        )
        x_lines = halves(x_lines)
        rows = slice(h * 128, (h + 1) * 128)
        add_cos = dot3(x_lines, (wx[0, rows], wx[1, rows]), NN)
        add_sin = dot3(x_lines, (wx[2, rows], wx[3, rows]), NN)
        with_cos = add_cos if h == 0 else with_cos + add_cos
        with_sin = add_sin if h == 0 else with_sin + add_sin
    spec_ref[0] = (with_cos[:128] + with_sin[128:]).reshape(16, 8, NXY)
    spec_ref[1] = (with_cos[128:] - with_sin[:128]).reshape(16, 8, NXY)
    for q in range(GZ):
        dens_ref[:, q * 8 : (q + 1) * 8, :] = dens_in[q].reshape(8, 8, 128)


def solution(mesh):
    wz = np.stack(np_halves(depth_matrix()))
    wxy = np.concatenate([np.stack(np_halves(m)) for m in plane_matrices()])
    wxy, wx = wxy[:4], wxy[4:]
    vmem = pl.BlockSpec(memory_space=pltpu.VMEM)
    far = pl.BlockSpec(memory_space=pltpu.HBM)
    dma = pltpu.SemaphoreType.DMA
    call = pl.pallas_call(
        kernel,
        out_shape=(
            pltpu.VMEM((GZ, 64, 128), F32),
            pltpu.VMEM((2, GX, 8, 128), F32),
        ),
        in_specs=[far] * 6 + [pl.BlockSpec(memory_space=pltpu.SMEM), far, far],
        out_specs=(vmem, vmem),
        scratch_shapes=[
            pltpu.VMEM((32, 529), F32),
            pltpu.VMEM((NPOLY, 529), F32),
            pltpu.VMEM((3, 32), jnp.int32),
            pltpu.VMEM((3, 32), F32),
            pltpu.VMEM((1, 32), jnp.int32),
            pltpu.VMEM((1, 32), jnp.int32),
            pltpu.VMEM((2, NZ, 2 * NZ), BF16),
            pltpu.VMEM((4, NXY, NXY), BF16),
            pltpu.VMEM((GX, 8, 128), F32),
            pltpu.VMEM((GX, 8, 128), F32),
            pltpu.VMEM((16, 8, SLOTS), F32),
            pltpu.VMEM((192, 4 * SLOTS), BF16),
            pltpu.VMEM((192, 4 * SLOTS), BF16),
            pltpu.VMEM((2, GROUPS, SLAB, 128), F32),
            pltpu.VMEM((2, GZ, SLAB, 128), F32),
            pltpu.VMEM((2, GZ, SLAB, 128), F32),
            pltpu.VMEM((GZ, 64, 128), F32),
            pltpu.VMEM((2, RING, 8, 128), F32),
            pltpu.VMEM((2, NXY, 128), F32),
            pltpu.VMEM((2, NXY, 128), F32),
            dma((8,)),
            dma, dma,
            dma((2,)), dma((2,)), dma((2,)),
            dma((2,)), dma((2,)),
            dma((2,)), dma((2,)),
            dma, dma,
        ],
        compiler_params=pltpu.CompilerParams(collective_id=0, has_side_effects=True),
        name="pair_grid_transform",
    )
    last = pl.pallas_call(
        last_kernel,
        out_shape=(
            jax.ShapeDtypeStruct((CX, CY, CZ), F32),
            jax.ShapeDtypeStruct((2, 16, 8, NXY), F32),
        ),
        in_specs=[vmem] * 3,
        out_specs=(vmem, vmem),
        compiler_params=pltpu.CompilerParams(vmem_limit_bytes=16 * 1024 * 1024),
        name="x_transform",
    )

    def shards(blocks, basis, cells, offsets, eidx, ridx, exps):
        dens, lines = call(
            blocks.T, basis.T, cells, offsets, eidx.reshape(1, -1), ridx.reshape(1, -1), exps,
            jnp.asarray(wz), jnp.asarray(wxy),
        )
        return last(dens, lines, jnp.asarray(wx))

    split = ("gx", "gy", "gz")
    placed = (P(None, split), P(), P(None, split), P(None, split), P(split), P(split), P())
    return jax.shard_map(
        shards,
        mesh=mesh,
        in_specs=placed,
        out_specs=(P("gx", "gy", "gz"), P(None, ("gy", "gz"), "gx", None)),
        check_vma=False,
    )
```

```python
import math

import jax
import jax.numpy as jnp
import ml_dtypes
import numpy as np
from jax import lax
from jax.experimental import pallas as pl
from jax.experimental.pallas import tpu as pltpu
from jax.sharding import PartitionSpec as P

HALO = 8
CX, CY, CZ = 8, 32, 128
GX, GY, GZ = 32, 8, 4
RING = GY * GZ
NZ = GZ * CZ
NXY = 256
SLOTS = GX * 8
GROUPS = 6
SLAB = 36
HX = 4
NPOLY = 64
MESH = pl.DeviceIdType.MESH
F32 = jnp.float32
BF16 = jnp.bfloat16

NN = (((1,), (0,)), ((), ()))
NT = (((1,), (1,)), ((), ()))


def halves(value):
    high = value.astype(BF16)
    return high, (value - high.astype(F32)).astype(BF16)


def dot(a, b, dims):
    return lax.dot_general(a, b, dims, preferred_element_type=F32)


def dot3(a, b, dims):
    rows = a[0].shape[0]
    both = dot(jnp.concatenate(a, 0), b[0], dims)
    return both[:rows] + (both[rows:] + dot(a[0], b[1], dims))


def unrolled(count):
    def run(body):
        for i in range(count):
            body(i)

    return run


def np_halves(value):
    value = value.astype(np.float32)
    high = value.astype(ml_dtypes.bfloat16)
    return high, (value - high.astype(np.float32)).astype(ml_dtypes.bfloat16)


def depth_matrix():
    lane = np.arange(128)
    kz = 16 * (8 * np.arange(4)[:, None] + lane[None, :] % 8) + lane[None, :] // 8
    phase = np.arange(NZ)[:, None] * kz.reshape(-1)[None, :] % NZ
    angle = phase * (2.0 * math.pi / NZ)
    scale = 1.0 / math.sqrt(NZ)
    return np.concatenate([np.cos(angle) * scale, -np.sin(angle) * scale], 1)


def plane_matrices():
    index = np.arange(NXY)
    angle = (index[:, None] * index[None, :] % NXY) * (2.0 * math.pi / NXY)
    scale = 1.0 / math.sqrt(NXY)
    order = np.arange(NXY).reshape(GX, 2, HX).transpose(1, 0, 2).reshape(-1)
    cosine, sine = np.cos(angle) * scale, np.sin(angle) * scale
    return cosine, sine, cosine[order], sine[order]


def iota(shape, axis):
    return lax.broadcasted_iota(jnp.int32, shape, axis)


def swap_lanes(v, count, group):
    bit = 1
    while bit < count:
        shift = bit * group
        v = v.reshape(count // (2 * bit), 2, bit * 8, 128)
        a = v[:, 0].reshape(count * 4, 128)
        c = v[:, 1].reshape(count * 4, 128)
        low = (iota((count * 4, 128), 1) // shift) % 2 == 0
        na = jnp.where(low, a, pltpu.roll(c, shift, 1))
        nc = jnp.where(low, pltpu.roll(a, 128 - shift, 1), c)
        parts = (count // (2 * bit), 1, bit * 8, 128)
        v = jnp.concatenate([na.reshape(parts), nc.reshape(parts)], 1)
        v = v.reshape(count, 8, 128)
        bit *= 2
    return v


def kernel(
    blocks_hbm, basis_hbm, cells_hbm, offsets_hbm, eidx_hbm, ridx_hbm, exps_ref,
    wz_hbm, wxy_hbm, dens_in, in5,
    blocks_ref, basis_ref, cells_ref, offsets_ref, eidx_ref, ridx_ref,
    wz, wxy, out1, recv1, amps, t_hi, t_lo, slabs, main_in, rim_in, lines,
    out4, in4, out5,
    wsem, s1, r1, s3, r3, r3x, s4, r4, s5, r5, sd, rd,
):
    gx, gy, gz = lax.axis_index("gx"), lax.axis_index("gy"), lax.axis_index("gz")
    me = gy * GZ + gz

    half, core = gz >> 1, gz & 1

    def far_first(i, reach):
        return (reach - (i + 1) // 2) * (2 * (i % 2) - 1)

    def plane_step(i):
        row = ((gx >> 2) + far_first(i // 4, 4)) & 7
        return row * 4 + (((gx & 3) + far_first(i % 4, 2)) & 3)

    def ring_step(i):
        depth = (gy + 8 * half + far_first(i // 2, 8)) & 15
        return (depth & 7) * GZ + (depth >> 3) * 2 + ((core + 1 + i) & 1)

    def arrived(ref, semaphore):
        pltpu.make_async_copy(ref, ref, semaphore).wait()

    def plane_peer(target):
        return {"gx": target}

    def ring_peer(target):
        return {"gy": target >> 2, "gz": target & 3}

    loads = [
        pltpu.make_async_copy(source, target, wsem.at[2 + n])
        for n, (source, target) in enumerate((
            (blocks_hbm, blocks_ref), (basis_hbm, basis_ref), (cells_hbm, cells_ref),
            (offsets_hbm, offsets_ref), (eidx_hbm, eidx_ref), (ridx_hbm, ridx_ref),
        ))
    ]
    for load in loads:
        load.start()
    wz_copy = pltpu.make_async_copy(wz_hbm, wz, wsem.at[0])
    wxy_copy = pltpu.make_async_copy(wxy_hbm, wxy, wsem.at[1])
    wz_copy.start()
    wxy_copy.start()

    barrier = pltpu.get_barrier_semaphore()

    @unrolled(GX - 1)
    def _(i):
        pl.semaphore_signal(
            barrier, inc=1, device_id=plane_peer(plane_step(i)), device_id_type=MESH
        )

    @unrolled(RING - 1)
    def _(i):
        pl.semaphore_signal(
            barrier, inc=1, device_id=ring_peer(ring_step(i)), device_id_type=MESH
        )

    for load in loads:
        load.wait()
    coefs = dot3(halves(basis_ref[...]), halves(blocks_ref[...]), NT)
    cells = cells_ref[...].astype(F32)
    radius = (HALO - ridx_ref[...]).astype(F32)
    rate = jnp.zeros((1, 32), F32)
    for e in range(16):
        rate = rate + jnp.where(eidx_ref[...] == e, exps_ref[e], 0.0)
    rate = rate / (radius * radius)
    data = jnp.concatenate(
        [coefs, cells, offsets_ref[...], rate, radius, jnp.zeros((56, 32), F32)], 0
    )
    owner = cells_ref[0:1, :] // CX
    same_pair = iota((32, 32), 0) == iota((32, 32), 1)
    owner_column = jnp.sum(
        jnp.where(same_pair, owner.astype(F32), 0.0), axis=1, keepdims=True
    ).astype(jnp.int32)
    earlier = (owner_column == owner) & (iota((32, 32), 0) < iota((32, 32), 1))
    within = jnp.sum(jnp.where(earlier, 1.0, 0.0), axis=0, keepdims=True).astype(jnp.int32)
    base = owner * 2 + within
    row = iota((SLOTS, 1), 0)
    slot = row % 8
    code = (row // 8 + slot // 2 + (GX - 1)) % GX * 2 + slot % 2
    code = jnp.where(slot < 6, code, -1)
    pick = jnp.where(code == base, 1.0, 0.0).astype(BF16)
    high, middle = halves(data)
    rest = (data - high.astype(F32) - middle.astype(F32)).astype(BF16)
    routed = dot(pick, high, NT) + dot(pick, middle, NT) + dot(pick, rest, NT)
    out1[...] = routed.reshape(GX, 8, 128)
    recv1[gx] = out1[gx]

    pl.semaphore_wait(barrier, GX + RING - 2)

    def copy1(target, source):
        return pltpu.make_async_remote_copy(
            src_ref=out1.at[target], dst_ref=recv1.at[source],
            send_sem=s1, recv_sem=r1,
            device_id=plane_peer(target), device_id_type=MESH,
        )

    @unrolled(GX - 1)
    def _(i):
        copy1(plane_step(i), gx).start()

    arrived(recv1.at[0 : GX - 1], r1)

    table = recv1[...].reshape(SLOTS, 128).T
    cx, cy, cz = table[64:65], table[65:66], table[66:67]
    ox, oy, oz = table[67:68], table[68:69], table[69:70]
    rates, radii = table[70:71], table[71:72]

    def factors(offset_cells, offset_in):
        distance = offset_cells - offset_in
        inside = jnp.abs(offset_cells) <= radii
        envelope = jnp.where(inside, jnp.exp(-rates * distance * distance), 0.0)
        scaled = distance * (1.0 / HALO)
        first = envelope * scaled
        second = first * scaled
        return [envelope, first, second, second * scaled]

    step_x = (gx * CX + iota((CX, 1), 0)).astype(F32) - cx
    step_x = jnp.where(step_x > 128.0, step_x - 256.0, step_x)
    step_x = jnp.where(step_x < -128.0, step_x + 256.0, step_x)
    along_x = factors(step_x, ox)
    for j in range(4):
        for k in range(4):
            total = table[j * 4 + k : j * 4 + k + 1] * along_x[0]
            for i in range(1, 4):
                at = i * 16 + j * 4 + k
                total = total + table[at : at + 1] * along_x[i]
            amps[j * 4 + k] = total
    along_y = factors((gy * CY - HALO + iota((48, 1), 0)).astype(F32) - cy, oy)
    z_row = iota((256, 1), 0)
    rim = z_row % 16
    z_cell = jnp.where(
        z_row < CZ, z_row, jnp.where(rim < HALO, CZ + rim, rim - 2 * HALO)
    )
    along_z = factors((gz * CZ + z_cell).astype(F32) - cz, oz)

    z_all = halves(jnp.concatenate(along_z, 1))
    keep = iota((8, 128), 1) // 16 == iota((8, 128), 0)

    def copy3(h, group, source):
        return pltpu.make_async_remote_copy(
            src_ref=slabs.at[h, group], dst_ref=main_in.at[h, source],
            send_sem=s3.at[h], recv_sem=r3.at[h],
            device_id={"gz": group - 1}, device_id_type=MESH,
        )

    def copy3_rim(h, group, source, row_to, depth_to):
        return pltpu.make_async_remote_copy(
            src_ref=slabs.at[h, group], dst_ref=rim_in.at[h, source],
            send_sem=s3.at[h], recv_sem=r3x.at[h],
            device_id={"gy": row_to, "gz": depth_to}, device_id_type=MESH,
        )

    before, after = lax.rem(gy + GY - 1, GY), lax.rem(gy + 1, GY)

    for h in range(2):
        for x in range(HX):
            for k in range(4):
                at = h * HX + x
                total = amps[k, at : at + 1, :] * along_y[0]
                for j in range(1, 4):
                    total = total + amps[j * 4 + k, at : at + 1, :] * along_y[j]
                high, low = halves(total)
                t_hi[x * 48 : (x + 1) * 48, k * SLOTS : (k + 1) * SLOTS] = high
                t_lo[x * 48 : (x + 1) * 48, k * SLOTS : (k + 1) * SLOTS] = low
        block = dot3((t_hi[...], t_lo[...]), z_all, NT)
        for x in range(HX):
            for g in range(GROUPS):
                at = x * 48 + g * 8
                slabs[h, g, x * 8 : (x + 1) * 8, :] = block[at : at + 8, :128]
                slabs[h, g, 32 + x : 33 + x, :] = jnp.sum(
                    jnp.where(keep, block[at : at + 8, 128:], 0.0), axis=0, keepdims=True
                )
        copy3(h, 3 - 2 * half + core, gz).start()
        copy3(h, 4 - 2 * half - core, gz).start()
        copy3_rim(h, 0, gz, before, GZ - 1).start()
        copy3_rim(h, 5, gz, after, 0).start()
        copy3(h, 2 + 2 * half - core, gz).start()
        main_in[h, gz] = slabs[h, 1 + gz]

    edge = (gz == 0) | (gz == GZ - 1)

    @pl.when(jnp.logical_not(edge))
    def _():
        rim_in[...] = jnp.zeros((2, GZ, SLAB, 128), F32)

    wz_copy.wait()
    wxy_copy.wait()

    def copy4(h, target, source):
        return pltpu.make_async_remote_copy(
            src_ref=out4.at[h, target],
            dst_ref=in4.at[h, pl.ds(pl.multiple_of(source * 8, 8), 8), :],
            send_sem=s4.at[h], recv_sem=r4.at[h],
            device_id=ring_peer(target), device_id_type=MESH,
        )

    def copy5(h, target, source):
        return pltpu.make_async_remote_copy(
            src_ref=out5.at[h, pl.ds(pl.multiple_of(target * 8, 8), 8), :],
            dst_ref=in5.at[h, source],
            send_sem=s5.at[h], recv_sem=r5.at[h],
            device_id=plane_peer(target), device_id_type=MESH,
        )

    def copy_d(target, source):
        return pltpu.make_async_remote_copy(
            src_ref=lines.at[target], dst_ref=dens_in.at[source],
            send_sem=sd, recv_sem=rd,
            device_id={"gz": target}, device_id_type=MESH,
        )

    row_lane = iota((32, 128), 1)
    keep_rows = row_lane // 16 == iota((32, 128), 0) % 8
    for h in range(2):
        arrived(main_in.at[h, 0 : GZ - 1], r3.at[h])

        @pl.when(edge)
        def _():
            arrived(rim_in.at[h], r3x.at[h])

        rims = []
        for q in range(GZ):
            packed = main_in[h, q, 32:SLAB, :] + rim_in[h, q, 32:SLAB, :]
            spread = jnp.concatenate(
                [jnp.broadcast_to(packed[x : x + 1], (8, 128)) for x in range(HX)], 0
            )
            spread = jnp.where(keep_rows, spread, 0.0)
            for shift in (16, 32, 64):
                spread = spread + pltpu.roll(spread, shift, 1)
            rims.append(spread)
        for q in range(GZ):
            lines[q, h * 32 : (h + 1) * 32, :] = (
                main_in[h, q, 0:32, :]
                + rim_in[h, q, 0:32, :]
                + jnp.where(row_lane >= CZ - HALO, rims[(q + 1) % GZ], 0.0)
                + jnp.where(row_lane < HALO, rims[(q + GZ - 1) % GZ], 0.0)
            )
        line_parts = halves(
            jnp.concatenate([lines[q, h * 32 : (h + 1) * 32, :] for q in range(GZ)], 1)
        )
        lines_hat = dot3(line_parts, (wz[0], wz[1]), NN)
        for c in range(4):
            pair = [lines_hat[:, p * 512 + c * 128 : p * 512 + (c + 1) * 128] for p in range(2)]
            part = jnp.concatenate([v.reshape(HX, 8, 128) for v in pair], 0)
            out4[h, c * 8 : (c + 1) * 8] = swap_lanes(part, 8, 1)

        @unrolled(RING - 1)
        def _(i):
            copy4(h, ring_step(i), me).start()

        in4[h, pl.ds(pl.multiple_of(me * 8, 8), 8), :] = out4[h, me]

    dens_in[gz] = lines[gz]

    cosines = (wxy[0], wxy[1])
    sines = (wxy[2], wxy[3])
    real_lane = iota((NXY, 128), 1) // HX % 2 == 0
    for h in range(2):
        arrived(in4.at[h, 0 : NXY - 8], r4.at[h])

        rows_in = halves(in4[h])
        with_cos = dot3(cosines, rows_in, NN)
        with_sin = dot3(sines, rows_in, NN)
        out5[h] = with_cos + jnp.where(
            real_lane, pltpu.roll(with_sin, 128 - HX, 1), -pltpu.roll(with_sin, HX, 1)
        )

        @unrolled(GX - 1)
        def _(i):
            copy5(h, plane_step(i), gx).start()

        in5[h, gx] = out5[h, pl.ds(pl.multiple_of(gx * 8, 8), 8), :]

        if h == 0:
            copy_d(2 - 2 * half + core, gz).start()
            copy_d(3 - 2 * half - core, gz).start()
            copy_d(2 * half + 1 - core, gz).start()

    for h in range(2):
        arrived(in5.at[h, 0 : GX - 1], r5.at[h])
    arrived(dens_in.at[0 : GZ - 1], rd)
    arrived(out1.at[0 : GX - 1], s1)
    arrived(lines.at[0 : GZ - 1], sd)
    for h in range(2):
        arrived(out5.at[h, 0 : NXY - 8], s5.at[h])
        arrived(out4.at[h, 0 : RING - 1], s4.at[h])
        arrived(slabs.at[h, 0 : GROUPS - 1], s3.at[h])


def last_kernel(dens_in, in5, wx, dens_ref, spec_ref):
    with_cos = with_sin = None
    for h in range(2):
        x_lines = swap_lanes(in5[h], 32, HX).reshape(16, 2, 8, 128)
        x_lines = jnp.concatenate(
            [x_lines[:, p].reshape(128, 128) for p in range(2)], 0
        )
        x_lines = halves(x_lines)
        rows = slice(h * 128, (h + 1) * 128)
        add_cos = dot3(x_lines, (wx[0, rows], wx[1, rows]), NN)
        add_sin = dot3(x_lines, (wx[2, rows], wx[3, rows]), NN)
        with_cos = add_cos if h == 0 else with_cos + add_cos
        with_sin = add_sin if h == 0 else with_sin + add_sin
    spec_ref[0] = (with_cos[:128] + with_sin[128:]).reshape(16, 8, NXY)
    spec_ref[1] = (with_cos[128:] - with_sin[:128]).reshape(16, 8, NXY)
    for q in range(GZ):
        dens_ref[:, q * 8 : (q + 1) * 8, :] = dens_in[q].reshape(8, 8, 128)


def solution(mesh):
    wz = np.stack(np_halves(depth_matrix()))
    wxy = np.concatenate([np.stack(np_halves(m)) for m in plane_matrices()])
    wxy, wx = wxy[:4], wxy[4:]
    vmem = pl.BlockSpec(memory_space=pltpu.VMEM)
    far = pl.BlockSpec(memory_space=pltpu.HBM)
    dma = pltpu.SemaphoreType.DMA
    call = pl.pallas_call(
        kernel,
        out_shape=(
            pltpu.VMEM((GZ, 64, 128), F32),
            pltpu.VMEM((2, GX, 8, 128), F32),
        ),
        in_specs=[far] * 6 + [pl.BlockSpec(memory_space=pltpu.SMEM), far, far],
        out_specs=(vmem, vmem),
        scratch_shapes=[
            pltpu.VMEM((32, 529), F32),
            pltpu.VMEM((NPOLY, 529), F32),
            pltpu.VMEM((3, 32), jnp.int32),
            pltpu.VMEM((3, 32), F32),
            pltpu.VMEM((1, 32), jnp.int32),
            pltpu.VMEM((1, 32), jnp.int32),
            pltpu.VMEM((2, NZ, 2 * NZ), BF16),
            pltpu.VMEM((4, NXY, NXY), BF16),
            pltpu.VMEM((GX, 8, 128), F32),
            pltpu.VMEM((GX, 8, 128), F32),
            pltpu.VMEM((16, 8, SLOTS), F32),
            pltpu.VMEM((192, 4 * SLOTS), BF16),
            pltpu.VMEM((192, 4 * SLOTS), BF16),
            pltpu.VMEM((2, GROUPS, SLAB, 128), F32),
            pltpu.VMEM((2, GZ, SLAB, 128), F32),
            pltpu.VMEM((2, GZ, SLAB, 128), F32),
            pltpu.VMEM((GZ, 64, 128), F32),
            pltpu.VMEM((2, RING, 8, 128), F32),
            pltpu.VMEM((2, NXY, 128), F32),
            pltpu.VMEM((2, NXY, 128), F32),
            dma((8,)),
            dma, dma,
            dma((2,)), dma((2,)), dma((2,)),
            dma((2,)), dma((2,)),
            dma((2,)), dma((2,)),
            dma, dma,
        ],
        compiler_params=pltpu.CompilerParams(collective_id=0, has_side_effects=True),
        name="pair_grid_transform",
    )
    last = pl.pallas_call(
        last_kernel,
        out_shape=(
            jax.ShapeDtypeStruct((CX, CY, CZ), F32),
            jax.ShapeDtypeStruct((2, 16, 8, NXY), F32),
        ),
        in_specs=[vmem] * 3,
        out_specs=(vmem, vmem),
        compiler_params=pltpu.CompilerParams(vmem_limit_bytes=16 * 1024 * 1024),
        name="x_transform",
    )

    def shards(blocks, basis, cells, offsets, eidx, ridx, exps):
        dens, lines = call(
            blocks.T, basis.T, cells, offsets, eidx.reshape(1, -1), ridx.reshape(1, -1), exps,
            jnp.asarray(wz), jnp.asarray(wxy),
        )
        return last(dens, lines, jnp.asarray(wx))

    split = ("gx", "gy", "gz")
    placed = (P(None, split), P(), P(None, split), P(None, split), P(split), P(split), P())
    return jax.shard_map(
        shards,
        mesh=mesh,
        in_specs=placed,
        out_specs=(P("gx", "gy", "gz"), P(None, ("gy", "gz"), "gx", None)),
        check_vma=False,
    )
```

```python
import math

import jax
import jax.numpy as jnp
import ml_dtypes
import numpy as np
from jax import lax
from jax.experimental import pallas as pl
from jax.experimental.pallas import tpu as pltpu
from jax.sharding import PartitionSpec as P

HALO = 8
CX, CY, CZ = 8, 32, 128
GX, GY, GZ = 32, 8, 4
RING = GY * GZ
NZ = GZ * CZ
NXY = 256
SLOTS = GX * 8
GROUPS = 6
SLAB = 36
HX = 4
NPOLY = 64
MESH = pl.DeviceIdType.MESH
F32 = jnp.float32
BF16 = jnp.bfloat16

NN = (((1,), (0,)), ((), ()))
NT = (((1,), (1,)), ((), ()))


def halves(value):
    high = value.astype(BF16)
    return high, (value - high.astype(F32)).astype(BF16)


def dot(a, b, dims):
    return lax.dot_general(a, b, dims, preferred_element_type=F32)


def dot3(a, b, dims):
    rows = a[0].shape[0]
    both = dot(jnp.concatenate(a, 0), b[0], dims)
    return both[:rows] + (both[rows:] + dot(a[0], b[1], dims))


def unrolled(count):
    def run(body):
        for i in range(count):
            body(i)

    return run


def np_halves(value):
    value = value.astype(np.float32)
    high = value.astype(ml_dtypes.bfloat16)
    return high, (value - high.astype(np.float32)).astype(ml_dtypes.bfloat16)


def depth_matrices():
    lane = np.arange(128)
    even = 16 * (16 * np.arange(2)[:, None] + lane[None, :] % 16) + lane[None, :] // 16 * 2
    scale = 1.0 / math.sqrt(NZ)
    for parity in range(2):
        phase = np.arange(NZ // 2)[:, None] * (even + parity).reshape(-1)[None, :] % NZ
        angle = phase * (2.0 * math.pi / NZ)
        yield np.concatenate([np.cos(angle) * scale, -np.sin(angle) * scale], 1)


def plane_matrices():
    index = np.arange(NXY)
    angle = (index[:, None] * index[None, :] % NXY) * (2.0 * math.pi / NXY)
    scale = 1.0 / math.sqrt(NXY)
    order = np.arange(NXY).reshape(GX, 2, HX).transpose(1, 0, 2).reshape(-1)
    cosine, sine = np.cos(angle) * scale, np.sin(angle) * scale
    return cosine, sine, cosine[order], sine[order]


def iota(shape, axis):
    return lax.broadcasted_iota(jnp.int32, shape, axis)


def swap_lanes(v, count, group):
    bit = 1
    while bit < count:
        shift = bit * group
        v = v.reshape(count // (2 * bit), 2, bit * 8, 128)
        a = v[:, 0].reshape(count * 4, 128)
        c = v[:, 1].reshape(count * 4, 128)
        low = (iota((count * 4, 128), 1) // shift) % 2 == 0
        na = jnp.where(low, a, pltpu.roll(c, shift, 1))
        nc = jnp.where(low, pltpu.roll(a, 128 - shift, 1), c)
        parts = (count // (2 * bit), 1, bit * 8, 128)
        v = jnp.concatenate([na.reshape(parts), nc.reshape(parts)], 1)
        v = v.reshape(count, 8, 128)
        bit *= 2
    return v


def kernel(
    blocks_hbm, basis_hbm, cells_hbm, offsets_hbm, eidx_hbm, ridx_hbm, exps_ref,
    wz_hbm, wxy_hbm, dens_in, in5,
    blocks_ref, basis_ref, cells_ref, offsets_ref, eidx_ref, ridx_ref,
    wz, wxy, out1, recv1, arrivals, amps, t_hi, t_lo, slabs, main_in, rim_in, lines,
    out4, in4, out5,
    wsem, s1, r1, s3, r3, r3x, s4, r4, s5, r5, sd, rd,
):
    gx, gy, gz = lax.axis_index("gx"), lax.axis_index("gy"), lax.axis_index("gz")
    me = gy * GZ + gz

    half, core = gz >> 1, gz & 1

    def far_first(i, reach):
        return (reach - (i + 1) // 2) * (2 * (i % 2) - 1)

    def plane_step(i):
        row = ((gx >> 2) + far_first(i // 4, 4)) & 7
        return row * 4 + (((gx & 3) + far_first(i % 4, 2)) & 3)

    def ring_step(i):
        depth = (gy + 8 * half + far_first(i // 2, 8)) & 15
        return (depth & 7) * GZ + (depth >> 3) * 2 + ((core + 1 + i) & 1)

    def arrived(ref, semaphore):
        pltpu.make_async_copy(ref, ref, semaphore).wait()

    def plane_peer(target):
        return {"gx": target}

    def ring_peer(target):
        return {"gy": target >> 2, "gz": target & 3}

    barrier = pltpu.get_barrier_semaphore()

    @unrolled(RING - 1)
    def _(i):
        pl.semaphore_signal(
            barrier, inc=1, device_id=ring_peer(ring_step(i)), device_id_type=MESH
        )

    @unrolled(GX - 1)
    def _(i):
        pl.semaphore_signal(
            barrier, inc=1, device_id=plane_peer(plane_step(i)), device_id_type=MESH
        )

    loads = [
        pltpu.make_async_copy(source, target, wsem.at[2 + n])
        for n, (source, target) in enumerate((
            (blocks_hbm, blocks_ref), (basis_hbm, basis_ref), (cells_hbm, cells_ref),
            (offsets_hbm, offsets_ref), (eidx_hbm, eidx_ref), (ridx_hbm, ridx_ref),
        ))
    ]
    for load in loads:
        load.start()
    wz_copy = pltpu.make_async_copy(wz_hbm, wz, wsem.at[0])
    wxy_copy = pltpu.make_async_copy(wxy_hbm, wxy, wsem.at[1])
    wz_copy.start()
    wxy_copy.start()

    for load in loads:
        load.wait()
    coefs = dot3(halves(basis_ref[...]), halves(blocks_ref[...]), NT)
    cells = cells_ref[...].astype(F32)
    radius = (HALO - ridx_ref[...]).astype(F32)
    rate = jnp.zeros((1, 32), F32)
    for e in range(16):
        rate = rate + jnp.where(eidx_ref[...] == e, exps_ref[e], 0.0)
    rate = rate / (radius * radius)
    data = jnp.concatenate(
        [coefs, cells, offsets_ref[...], rate, radius, jnp.zeros((56, 32), F32)], 0
    )
    owner = cells_ref[0:1, :] // CX
    same_pair = iota((32, 32), 0) == iota((32, 32), 1)
    owner_column = jnp.sum(
        jnp.where(same_pair, owner.astype(F32), 0.0), axis=1, keepdims=True
    ).astype(jnp.int32)
    earlier = (owner_column == owner) & (iota((32, 32), 0) < iota((32, 32), 1))
    within = jnp.sum(jnp.where(earlier, 1.0, 0.0), axis=0, keepdims=True).astype(jnp.int32)
    base = owner * 2 + within
    row = iota((4 * GX, 1), 0)
    turn = row % 4
    pieces = halves(data)
    rest = (data - pieces[0].astype(F32) - pieces[1].astype(F32)).astype(BF16)
    chosen = []
    for side in range(2):
        code = (row // 4 + turn + (GX - 1)) % GX * 2 + side
        code = jnp.where(turn < 3, code, -1)
        pick = jnp.where(code == base, 1.0, 0.0).astype(BF16)
        chosen.append(
            dot(pick, pieces[0], NT) + dot(pick, pieces[1], NT) + dot(pick, rest, NT)
        )
    lane = iota((4 * GX, 128), 1)
    packed = jnp.where(lane < 64, chosen[0], pltpu.roll(chosen[1], 64, 1))
    labels = jnp.zeros((4 * GX, 128), F32)
    for r in range(3):
        for side in range(2):
            spot = r * 16 + side * 8
            moved = pltpu.roll(pltpu.roll(chosen[side], 64 + spot, 1), 3 - r, 0)
            labels = jnp.where((lane >= spot) & (lane < spot + 8), moved, labels)
    packed = jnp.where(iota((4 * GX, 128), 0) % 4 == 3, labels, packed)
    for target in range(GX):
        out1[target] = packed[target * 4 : (target + 1) * 4, :]
    recv1[gx] = out1[gx]

    pl.semaphore_wait(barrier, GX + RING - 2)

    def copy1(target, source):
        return pltpu.make_async_remote_copy(
            src_ref=out1.at[target], dst_ref=recv1.at[source],
            send_sem=s1, recv_sem=r1,
            device_id=plane_peer(target), device_id_type=MESH,
        )

    @unrolled(GX - 1)
    def _(i):
        copy1(plane_step(i), gx).start()

    arrived(recv1.at[0 : GX - 1], r1)

    for source in range(GX):
        arrivals[source * 4 : (source + 1) * 4, :] = recv1[source]
    turned = arrivals[...].T
    column = iota((1, 128), 1) % 4
    table = jnp.concatenate(
        [jnp.where(column < 3, turned[side * 64 : side * 64 + 64], 0.0) for side in range(2)], 1
    )
    labels = []
    for side in range(2):
        own = jnp.zeros((8, 128), F32)
        for r in range(3):
            spot = r * 16 + side * 8
            moved = pltpu.roll(turned[spot : spot + 8], 125 + r, 1)
            own = jnp.where(column == r, moved, own)
        labels.append(own)
    labels = jnp.concatenate(labels, 1)
    cx, cy, cz = labels[0:1], labels[1:2], labels[2:3]
    ox, oy, oz = labels[3:4], labels[4:5], labels[5:6]
    rates, radii = labels[6:7], labels[7:8]

    def factors(offset_cells, offset_in):
        distance = offset_cells - offset_in
        inside = jnp.abs(offset_cells) <= radii
        envelope = jnp.where(inside, jnp.exp(-rates * distance * distance), 0.0)
        scaled = distance * (1.0 / HALO)
        first = envelope * scaled
        second = first * scaled
        return [envelope, first, second, second * scaled]

    step_x = (gx * CX + iota((CX, 1), 0)).astype(F32) - cx
    step_x = jnp.where(step_x > 128.0, step_x - 256.0, step_x)
    step_x = jnp.where(step_x < -128.0, step_x + 256.0, step_x)
    along_x = factors(step_x, ox)
    for j in range(4):
        for k in range(4):
            total = table[j * 4 + k : j * 4 + k + 1] * along_x[0]
            for i in range(1, 4):
                at = i * 16 + j * 4 + k
                total = total + table[at : at + 1] * along_x[i]
            amps[j * 4 + k] = total
    along_y = factors((gy * CY - HALO + iota((48, 1), 0)).astype(F32) - cy, oy)
    z_row = iota((256, 1), 0)
    rim = z_row % 16
    z_cell = jnp.where(
        z_row < CZ, z_row, jnp.where(rim < HALO, CZ + rim, rim - 2 * HALO)
    )
    along_z = factors((gz * CZ + z_cell).astype(F32) - cz, oz)

    z_all = halves(jnp.concatenate(along_z, 1))
    keep = iota((8, 128), 1) // 16 == iota((8, 128), 0)

    def copy3(h, group, source):
        return pltpu.make_async_remote_copy(
            src_ref=slabs.at[h, group], dst_ref=main_in.at[h, source],
            send_sem=s3.at[h], recv_sem=r3.at[h],
            device_id={"gz": group - 1}, device_id_type=MESH,
        )

    def copy3_rim(h, group, source, row_to, depth_to):
        return pltpu.make_async_remote_copy(
            src_ref=slabs.at[h, group], dst_ref=rim_in.at[h, source],
            send_sem=s3.at[h], recv_sem=r3x.at[h],
            device_id={"gy": row_to, "gz": depth_to}, device_id_type=MESH,
        )

    before, after = lax.rem(gy + GY - 1, GY), lax.rem(gy + 1, GY)

    for h in range(2):
        for x in range(HX):
            for k in range(4):
                at = h * HX + x
                total = amps[k, at : at + 1, :] * along_y[0]
                for j in range(1, 4):
                    total = total + amps[j * 4 + k, at : at + 1, :] * along_y[j]
                high, low = halves(total)
                t_hi[x * 48 : (x + 1) * 48, k * SLOTS : (k + 1) * SLOTS] = high
                t_lo[x * 48 : (x + 1) * 48, k * SLOTS : (k + 1) * SLOTS] = low
        block = dot3((t_hi[...], t_lo[...]), z_all, NT)
        for x in range(HX):
            for g in range(GROUPS):
                at = x * 48 + g * 8
                slabs[h, g, x * 8 : (x + 1) * 8, :] = block[at : at + 8, :128]
                slabs[h, g, 32 + x : 33 + x, :] = jnp.sum(
                    jnp.where(keep, block[at : at + 8, 128:], 0.0), axis=0, keepdims=True
                )
        copy3(h, 3 - 2 * half + core, gz).start()
        copy3(h, 4 - 2 * half - core, gz).start()
        copy3_rim(h, 0, gz, before, GZ - 1).start()
        copy3_rim(h, 5, gz, after, 0).start()
        copy3(h, 2 + 2 * half - core, gz).start()
        main_in[h, gz] = slabs[h, 1 + gz]

    edge = (gz == 0) | (gz == GZ - 1)

    @pl.when(jnp.logical_not(edge))
    def _():
        rim_in[...] = jnp.zeros((2, GZ, SLAB, 128), F32)

    wz_copy.wait()
    wxy_copy.wait()

    def copy4(h, target, source):
        return pltpu.make_async_remote_copy(
            src_ref=out4.at[h, target],
            dst_ref=in4.at[h, pl.ds(pl.multiple_of(source * 8, 8), 8), :],
            send_sem=s4.at[h], recv_sem=r4.at[h],
            device_id=ring_peer(target), device_id_type=MESH,
        )

    def copy5(h, target, source):
        return pltpu.make_async_remote_copy(
            src_ref=out5.at[h, pl.ds(pl.multiple_of(target * 8, 8), 8), :],
            dst_ref=in5.at[h, source],
            send_sem=s5.at[h], recv_sem=r5.at[h],
            device_id=plane_peer(target), device_id_type=MESH,
        )

    def copy_d(target, source):
        return pltpu.make_async_remote_copy(
            src_ref=lines.at[target], dst_ref=dens_in.at[source],
            send_sem=sd, recv_sem=rd,
            device_id={"gz": target}, device_id_type=MESH,
        )

    row_lane = iota((32, 128), 1)
    keep_rows = row_lane // 16 == iota((32, 128), 0) % 8
    for h in range(2):
        arrived(main_in.at[h, 0 : GZ - 1], r3.at[h])

        @pl.when(edge)
        def _():
            arrived(rim_in.at[h], r3x.at[h])

        rims = []
        for q in range(GZ):
            packed = main_in[h, q, 32:SLAB, :] + rim_in[h, q, 32:SLAB, :]
            spread = jnp.concatenate(
                [jnp.broadcast_to(packed[x : x + 1], (8, 128)) for x in range(HX)], 0
            )
            spread = jnp.where(keep_rows, spread, 0.0)
            for shift in (16, 32, 64):
                spread = spread + pltpu.roll(spread, shift, 1)
            rims.append(spread)
        for q in range(GZ):
            lines[q, h * 32 : (h + 1) * 32, :] = (
                main_in[h, q, 0:32, :]
                + rim_in[h, q, 0:32, :]
                + jnp.where(row_lane >= CZ - HALO, rims[(q + 1) % GZ], 0.0)
                + jnp.where(row_lane < HALO, rims[(q + GZ - 1) % GZ], 0.0)
            )
        near = [lines[q, h * 32 : (h + 1) * 32, :] for q in range(GZ)]
        sums = jnp.concatenate([near[0] + near[2], near[1] + near[3]], 1)
        gaps = jnp.concatenate([near[0] - near[2], near[1] - near[3]], 1)
        even = dot3(halves(sums), (wz[0], wz[1]), NN)
        odd = dot3(halves(gaps), (wz[2], wz[3]), NN)
        for c in range(2):
            part = jnp.concatenate(
                [
                    v[:, p * 256 + c * 128 : p * 256 + (c + 1) * 128].reshape(HX, 8, 128)
                    for v in (even, odd)
                    for p in range(2)
                ],
                0,
            )
            out4[h, c * 16 : (c + 1) * 16] = swap_lanes(part, 16, 1)

        @unrolled(RING - 1)
        def _(i):
            copy4(h, ring_step(i), me).start()

        in4[h, pl.ds(pl.multiple_of(me * 8, 8), 8), :] = out4[h, me]

    dens_in[gz] = lines[gz]

    cosines = (wxy[0], wxy[1])
    sines = (wxy[2], wxy[3])
    real_lane = iota((NXY, 128), 1) // HX % 2 == 0
    for h in range(2):
        arrived(in4.at[h, 0 : NXY - 8], r4.at[h])

        rows_in = halves(in4[h])
        with_cos = dot3(cosines, rows_in, NN)
        with_sin = dot3(sines, rows_in, NN)
        out5[h] = with_cos + jnp.where(
            real_lane, pltpu.roll(with_sin, 128 - HX, 1), -pltpu.roll(with_sin, HX, 1)
        )

        @unrolled(GX - 1)
        def _(i):
            copy5(h, plane_step(i), gx).start()

        in5[h, gx] = out5[h, pl.ds(pl.multiple_of(gx * 8, 8), 8), :]

        if h == 0:
            copy_d(2 - 2 * half + core, gz).start()
            copy_d(3 - 2 * half - core, gz).start()
            copy_d(2 * half + 1 - core, gz).start()

    for h in range(2):
        arrived(in5.at[h, 0 : GX - 1], r5.at[h])
    arrived(dens_in.at[0 : GZ - 1], rd)
    arrived(out1.at[0 : GX - 1], s1)
    arrived(lines.at[0 : GZ - 1], sd)
    for h in range(2):
        arrived(out5.at[h, 0 : NXY - 8], s5.at[h])
        arrived(out4.at[h, 0 : RING - 1], s4.at[h])
        arrived(slabs.at[h, 0 : GROUPS - 1], s3.at[h])


def last_kernel(dens_in, in5, wx, dens_ref, spec_ref):
    with_cos = with_sin = None
    for h in range(2):
        x_lines = swap_lanes(in5[h], 32, HX).reshape(16, 2, 8, 128)
        x_lines = jnp.concatenate(
            [x_lines[:, p].reshape(128, 128) for p in range(2)], 0
        )
        x_lines = halves(x_lines)
        rows = slice(h * 128, (h + 1) * 128)
        add_cos = dot3(x_lines, (wx[0, rows], wx[1, rows]), NN)
        add_sin = dot3(x_lines, (wx[2, rows], wx[3, rows]), NN)
        with_cos = add_cos if h == 0 else with_cos + add_cos
        with_sin = add_sin if h == 0 else with_sin + add_sin
    spec_ref[0] = (with_cos[:128] + with_sin[128:]).reshape(16, 8, NXY)
    spec_ref[1] = (with_cos[128:] - with_sin[:128]).reshape(16, 8, NXY)
    for q in range(GZ):
        dens_ref[:, q * 8 : (q + 1) * 8, :] = dens_in[q].reshape(8, 8, 128)


def solution(mesh):
    wz = np.concatenate([np.stack(np_halves(m)) for m in depth_matrices()])
    wxy = np.concatenate([np.stack(np_halves(m)) for m in plane_matrices()])
    wxy, wx = wxy[:4], wxy[4:]
    vmem = pl.BlockSpec(memory_space=pltpu.VMEM)
    far = pl.BlockSpec(memory_space=pltpu.HBM)
    dma = pltpu.SemaphoreType.DMA
    call = pl.pallas_call(
        kernel,
        out_shape=(
            pltpu.VMEM((GZ, 64, 128), F32),
            pltpu.VMEM((2, GX, 8, 128), F32),
        ),
        in_specs=[far] * 6 + [pl.BlockSpec(memory_space=pltpu.SMEM), far, far],
        out_specs=(vmem, vmem),
        scratch_shapes=[
            pltpu.VMEM((32, 529), F32),
            pltpu.VMEM((NPOLY, 529), F32),
            pltpu.VMEM((3, 32), jnp.int32),
            pltpu.VMEM((3, 32), F32),
            pltpu.VMEM((1, 32), jnp.int32),
            pltpu.VMEM((1, 32), jnp.int32),
            pltpu.VMEM((4, NZ // 2, NZ), BF16),
            pltpu.VMEM((4, NXY, NXY), BF16),
            pltpu.VMEM((GX, 4, 128), F32),
            pltpu.VMEM((GX, 4, 128), F32),
            pltpu.VMEM((4 * GX, 128), F32),
            pltpu.VMEM((16, 8, SLOTS), F32),
            pltpu.VMEM((192, 4 * SLOTS), BF16),
            pltpu.VMEM((192, 4 * SLOTS), BF16),
            pltpu.VMEM((2, GROUPS, SLAB, 128), F32),
            pltpu.VMEM((2, GZ, SLAB, 128), F32),
            pltpu.VMEM((2, GZ, SLAB, 128), F32),
            pltpu.VMEM((GZ, 64, 128), F32),
            pltpu.VMEM((2, RING, 8, 128), F32),
            pltpu.VMEM((2, NXY, 128), F32),
            pltpu.VMEM((2, NXY, 128), F32),
            dma((8,)),
            dma, dma,
            dma((2,)), dma((2,)), dma((2,)),
            dma((2,)), dma((2,)),
            dma((2,)), dma((2,)),
            dma, dma,
        ],
        compiler_params=pltpu.CompilerParams(collective_id=0, has_side_effects=True),
        name="pair_grid_transform",
    )
    last = pl.pallas_call(
        last_kernel,
        out_shape=(
            jax.ShapeDtypeStruct((CX, CY, CZ), F32),
            jax.ShapeDtypeStruct((2, 16, 8, NXY), F32),
        ),
        in_specs=[vmem] * 3,
        out_specs=(vmem, vmem),
        compiler_params=pltpu.CompilerParams(vmem_limit_bytes=16 * 1024 * 1024),
        name="x_transform",
    )

    def shards(blocks, basis, cells, offsets, eidx, ridx, exps):
        dens, lines = call(
            blocks.T, basis.T, cells, offsets, eidx.reshape(1, -1), ridx.reshape(1, -1), exps,
            jnp.asarray(wz), jnp.asarray(wxy),
        )
        return last(dens, lines, jnp.asarray(wx))

    split = ("gx", "gy", "gz")
    placed = (P(None, split), P(), P(None, split), P(None, split), P(split), P(split), P())
    return jax.shard_map(
        shards,
        mesh=mesh,
        in_specs=placed,
        out_specs=(P("gx", "gy", "gz"), P(None, ("gy", "gz"), "gx", None)),
        check_vma=False,
    )
```

```python
import math

import jax
import jax.numpy as jnp
import ml_dtypes
import numpy as np
from jax import lax
from jax.experimental import pallas as pl
from jax.experimental.pallas import tpu as pltpu
from jax.sharding import PartitionSpec as P

HALO = 8
CX, CY, CZ = 8, 32, 128
GX, GY, GZ = 32, 8, 4
RING = GY * GZ
NZ = GZ * CZ
NXY = 256
SLOTS = GX * 8
GROUPS = 6
SLAB = 36
HX = 4
NPOLY = 64
MESH = pl.DeviceIdType.MESH
F32 = jnp.float32
BF16 = jnp.bfloat16

NN = (((1,), (0,)), ((), ()))
NT = (((1,), (1,)), ((), ()))


def halves(value):
    high = value.astype(BF16)
    return high, (value - high.astype(F32)).astype(BF16)


def dot(a, b, dims):
    return lax.dot_general(a, b, dims, preferred_element_type=F32)


def dot3(a, b, dims):
    rows = a[0].shape[0]
    both = dot(jnp.concatenate(a, 0), b[0], dims)
    return both[:rows] + (both[rows:] + dot(a[0], b[1], dims))


def unrolled(count):
    def run(body):
        for i in range(count):
            body(i)

    return run


def np_halves(value):
    value = value.astype(np.float32)
    high = value.astype(ml_dtypes.bfloat16)
    return high, (value - high.astype(np.float32)).astype(ml_dtypes.bfloat16)


def depth_matrices():
    lane = np.arange(128)
    even = 16 * (16 * np.arange(2)[:, None] + lane[None, :] % 16) + lane[None, :] // 16 * 2
    scale = 1.0 / math.sqrt(NZ)
    for parity in range(2):
        phase = np.arange(NZ // 2)[:, None] * (even + parity).reshape(-1)[None, :] % NZ
        angle = phase * (2.0 * math.pi / NZ)
        yield np.concatenate([np.cos(angle) * scale, -np.sin(angle) * scale], 1)


def plane_matrices():
    index = np.arange(NXY)
    angle = (index[:, None] * index[None, :] % NXY) * (2.0 * math.pi / NXY)
    scale = 1.0 / math.sqrt(NXY)
    order = np.arange(NXY).reshape(GX, 2, HX).transpose(1, 0, 2).reshape(-1)
    cosine, sine = np.cos(angle) * scale, np.sin(angle) * scale
    return cosine, sine, cosine[order], sine[order]


def iota(shape, axis):
    return lax.broadcasted_iota(jnp.int32, shape, axis)


def swap_lanes(v, count, group):
    bit = 1
    while bit < count:
        shift = bit * group
        v = v.reshape(count // (2 * bit), 2, bit * 8, 128)
        a = v[:, 0].reshape(count * 4, 128)
        c = v[:, 1].reshape(count * 4, 128)
        low = (iota((count * 4, 128), 1) // shift) % 2 == 0
        na = jnp.where(low, a, pltpu.roll(c, shift, 1))
        nc = jnp.where(low, pltpu.roll(a, 128 - shift, 1), c)
        parts = (count // (2 * bit), 1, bit * 8, 128)
        v = jnp.concatenate([na.reshape(parts), nc.reshape(parts)], 1)
        v = v.reshape(count, 8, 128)
        bit *= 2
    return v


def kernel(
    blocks_hbm, basis_hbm, cells_hbm, offsets_hbm, eidx_hbm, ridx_hbm, exps_ref,
    wz_hbm, wxy_hbm, dens_in, in5,
    blocks_ref, basis_ref, cells_ref, offsets_ref, eidx_ref, ridx_ref,
    wz, wxy, out1, recv1, arrivals, amps, t_hi, t_lo, slabs, main_in, rim_in, lines,
    out4, in4, out5,
    wsem, s1, r1, s3, r3, r3x, s4, r4, s5, r5, sd, rd,
):
    gx, gy, gz = lax.axis_index("gx"), lax.axis_index("gy"), lax.axis_index("gz")
    me = gy * GZ + gz

    half, core = gz >> 1, gz & 1

    def far_first(i, reach):
        return (reach - (i + 1) // 2) * (2 * (i % 2) - 1)

    def plane_step(i):
        row = ((gx >> 2) + far_first(i // 4, 4)) & 7
        return row * 4 + (((gx & 3) + far_first(i % 4, 2)) & 3)

    def ring_step(i):
        depth = (gy + 8 * half + far_first(i // 2, 8)) & 15
        return (depth & 7) * GZ + (depth >> 3) * 2 + ((core + 1 + i) & 1)

    def arrived(ref, semaphore):
        pltpu.make_async_copy(ref, ref, semaphore).wait()

    def plane_peer(target):
        return {"gx": target}

    def ring_peer(target):
        return {"gy": target >> 2, "gz": target & 3}

    barrier = pltpu.get_barrier_semaphore()

    @unrolled(RING - 1)
    def _(i):
        pl.semaphore_signal(
            barrier, inc=1, device_id=ring_peer(ring_step(i)), device_id_type=MESH
        )

    @unrolled(GX - 1)
    def _(i):
        pl.semaphore_signal(
            barrier, inc=1, device_id=plane_peer(plane_step(i)), device_id_type=MESH
        )

    loads = [
        pltpu.make_async_copy(source, target, wsem.at[2 + n])
        for n, (source, target) in enumerate((
            (blocks_hbm, blocks_ref), (basis_hbm, basis_ref), (cells_hbm, cells_ref),
            (offsets_hbm, offsets_ref), (eidx_hbm, eidx_ref), (ridx_hbm, ridx_ref),
        ))
    ]
    for load in loads:
        load.start()
    wz_copy = pltpu.make_async_copy(wz_hbm, wz, wsem.at[0])
    wxy_copy = pltpu.make_async_copy(wxy_hbm, wxy, wsem.at[1])
    wz_copy.start()
    wxy_copy.start()

    for load in loads:
        load.wait()
    coefs = dot3(halves(basis_ref[...]), halves(blocks_ref[...]), NT)
    cells = cells_ref[...].astype(F32)
    radius = (HALO - ridx_ref[...]).astype(F32)
    rate = jnp.zeros((1, 32), F32)
    for e in range(16):
        rate = rate + jnp.where(eidx_ref[...] == e, exps_ref[e], 0.0)
    rate = rate / (radius * radius)
    data = jnp.concatenate(
        [coefs, cells, offsets_ref[...], rate, radius, jnp.zeros((56, 32), F32)], 0
    )
    owner = cells_ref[0:1, :] // CX
    same_pair = iota((32, 32), 0) == iota((32, 32), 1)
    owner_column = jnp.sum(
        jnp.where(same_pair, owner.astype(F32), 0.0), axis=1, keepdims=True
    ).astype(jnp.int32)
    earlier = (owner_column == owner) & (iota((32, 32), 0) < iota((32, 32), 1))
    within = jnp.sum(jnp.where(earlier, 1.0, 0.0), axis=0, keepdims=True).astype(jnp.int32)
    base = owner * 2 + within
    row = iota((4 * GX, 1), 0)
    turn = row % 4
    pieces = halves(data)
    rest = (data - pieces[0].astype(F32) - pieces[1].astype(F32)).astype(BF16)
    chosen = []
    for side in range(2):
        code = (row // 4 + turn + (GX - 1)) % GX * 2 + side
        code = jnp.where(turn < 3, code, -1)
        pick = jnp.where(code == base, 1.0, 0.0).astype(BF16)
        chosen.append(
            dot(pick, pieces[0], NT) + dot(pick, pieces[1], NT) + dot(pick, rest, NT)
        )
    lane = iota((4 * GX, 128), 1)
    packed = jnp.where(lane < 64, chosen[0], pltpu.roll(chosen[1], 64, 1))
    labels = jnp.zeros((4 * GX, 128), F32)
    for r in range(3):
        for side in range(2):
            spot = r * 16 + side * 8
            moved = pltpu.roll(pltpu.roll(chosen[side], 64 + spot, 1), 3 - r, 0)
            labels = jnp.where((lane >= spot) & (lane < spot + 8), moved, labels)
    packed = jnp.where(iota((4 * GX, 128), 0) % 4 == 3, labels, packed)
    for target in range(GX):
        out1[target] = packed[target * 4 : (target + 1) * 4, :]
    recv1[gx] = out1[gx]

    pl.semaphore_wait(barrier, GX + RING - 2)

    def copy1(target, source):
        return pltpu.make_async_remote_copy(
            src_ref=out1.at[target], dst_ref=recv1.at[source],
            send_sem=s1, recv_sem=r1,
            device_id=plane_peer(target), device_id_type=MESH,
        )

    @unrolled(GX - 1)
    def _(i):
        copy1(plane_step(i), gx).start()

    arrived(recv1.at[0 : GX - 1], r1)

    for source in range(GX):
        arrivals[source * 4 : (source + 1) * 4, :] = recv1[source]
    turned = arrivals[...].T
    column = iota((1, 128), 1) % 4
    table = jnp.concatenate(
        [jnp.where(column < 3, turned[side * 64 : side * 64 + 64], 0.0) for side in range(2)], 1
    )
    labels = []
    for side in range(2):
        own = jnp.zeros((8, 128), F32)
        for r in range(3):
            spot = r * 16 + side * 8
            moved = pltpu.roll(turned[spot : spot + 8], 125 + r, 1)
            own = jnp.where(column == r, moved, own)
        labels.append(own)
    labels = jnp.concatenate(labels, 1)
    cx, cy, cz = labels[0:1], labels[1:2], labels[2:3]
    ox, oy, oz = labels[3:4], labels[4:5], labels[5:6]
    rates, radii = labels[6:7], labels[7:8]

    def factors(offset_cells, offset_in):
        distance = offset_cells - offset_in
        inside = jnp.abs(offset_cells) <= radii
        envelope = jnp.where(inside, jnp.exp(-rates * distance * distance), 0.0)
        scaled = distance * (1.0 / HALO)
        first = envelope * scaled
        second = first * scaled
        return [envelope, first, second, second * scaled]

    step_x = (gx * CX + iota((CX, 1), 0)).astype(F32) - cx
    step_x = jnp.where(step_x > 128.0, step_x - 256.0, step_x)
    step_x = jnp.where(step_x < -128.0, step_x + 256.0, step_x)
    along_x = factors(step_x, ox)
    for j in range(4):
        for k in range(4):
            total = table[j * 4 + k : j * 4 + k + 1] * along_x[0]
            for i in range(1, 4):
                at = i * 16 + j * 4 + k
                total = total + table[at : at + 1] * along_x[i]
            amps[j * 4 + k] = total
    along_y = factors((gy * CY - HALO + iota((48, 1), 0)).astype(F32) - cy, oy)
    z_row = iota((256, 1), 0)
    rim = z_row % 16
    z_cell = jnp.where(
        z_row < CZ, z_row, jnp.where(rim < HALO, CZ + rim, rim - 2 * HALO)
    )
    along_z = factors((gz * CZ + z_cell).astype(F32) - cz, oz)

    z_all = halves(jnp.concatenate(along_z, 1))
    keep = iota((8, 128), 1) // 16 == iota((8, 128), 0)

    def copy3(h, group, source):
        return pltpu.make_async_remote_copy(
            src_ref=slabs.at[h, group], dst_ref=main_in.at[h, source],
            send_sem=s3.at[h], recv_sem=r3.at[h],
            device_id={"gz": group - 1}, device_id_type=MESH,
        )

    def copy3_rim(h, group, source, row_to, depth_to):
        return pltpu.make_async_remote_copy(
            src_ref=slabs.at[h, group], dst_ref=rim_in.at[h, source],
            send_sem=s3.at[h], recv_sem=r3x.at[h],
            device_id={"gy": row_to, "gz": depth_to}, device_id_type=MESH,
        )

    before, after = lax.rem(gy + GY - 1, GY), lax.rem(gy + 1, GY)
    far_row = jnp.where(half == 0, before, after)
    near_row = jnp.where(half == 0, after, before)

    for h in range(2):
        for x in range(HX):
            for k in range(4):
                at = h * HX + x
                total = amps[k, at : at + 1, :] * along_y[0]
                for j in range(1, 4):
                    total = total + amps[j * 4 + k, at : at + 1, :] * along_y[j]
                high, low = halves(total)
                t_hi[x * 48 : (x + 1) * 48, k * SLOTS : (k + 1) * SLOTS] = high
                t_lo[x * 48 : (x + 1) * 48, k * SLOTS : (k + 1) * SLOTS] = low
        block = dot3((t_hi[...], t_lo[...]), z_all, NT)
        for x in range(HX):
            for g in range(GROUPS):
                at = x * 48 + g * 8
                slabs[h, g, x * 8 : (x + 1) * 8, :] = block[at : at + 8, :128]
                slabs[h, g, 32 + x : 33 + x, :] = jnp.sum(
                    jnp.where(keep, block[at : at + 8, 128:], 0.0), axis=0, keepdims=True
                )
        copy3(h, 3 - 2 * half + core, gz).start()
        copy3(h, 4 - 2 * half - core, gz).start()
        copy3_rim(h, 5 * half, gz, far_row, (1 - half) * (GZ - 1)).start()
        copy3_rim(h, 5 - 5 * half, gz, near_row, half * (GZ - 1)).start()
        copy3(h, 2 + 2 * half - core, gz).start()
        main_in[h, gz] = slabs[h, 1 + gz]

    edge = (gz == 0) | (gz == GZ - 1)

    @pl.when(jnp.logical_not(edge))
    def _():
        rim_in[...] = jnp.zeros((2, GZ, SLAB, 128), F32)

    wz_copy.wait()
    wxy_copy.wait()

    def copy4(h, target, source):
        return pltpu.make_async_remote_copy(
            src_ref=out4.at[h, target],
            dst_ref=in4.at[h, pl.ds(pl.multiple_of(source * 8, 8), 8), :],
            send_sem=s4.at[h], recv_sem=r4.at[h],
            device_id=ring_peer(target), device_id_type=MESH,
        )

    def copy5(h, target, source):
        return pltpu.make_async_remote_copy(
            src_ref=out5.at[h, pl.ds(pl.multiple_of(target * 8, 8), 8), :],
            dst_ref=in5.at[h, source],
            send_sem=s5.at[h], recv_sem=r5.at[h],
            device_id=plane_peer(target), device_id_type=MESH,
        )

    def copy_d(target, source):
        return pltpu.make_async_remote_copy(
            src_ref=lines.at[target], dst_ref=dens_in.at[source],
            send_sem=sd, recv_sem=rd,
            device_id={"gz": target}, device_id_type=MESH,
        )

    row_lane = iota((32, 128), 1)
    keep_rows = row_lane // 16 == iota((32, 128), 0) % 8
    for h in range(2):
        arrived(main_in.at[h, 0 : GZ - 1], r3.at[h])

        @pl.when(edge)
        def _():
            arrived(rim_in.at[h], r3x.at[h])

        rims = []
        for q in range(GZ):
            packed = main_in[h, q, 32:SLAB, :] + rim_in[h, q, 32:SLAB, :]
            spread = jnp.concatenate(
                [jnp.broadcast_to(packed[x : x + 1], (8, 128)) for x in range(HX)], 0
            )
            spread = jnp.where(keep_rows, spread, 0.0)
            for shift in (16, 32, 64):
                spread = spread + pltpu.roll(spread, shift, 1)
            rims.append(spread)
        for q in range(GZ):
            lines[q, h * 32 : (h + 1) * 32, :] = (
                main_in[h, q, 0:32, :]
                + rim_in[h, q, 0:32, :]
                + jnp.where(row_lane >= CZ - HALO, rims[(q + 1) % GZ], 0.0)
                + jnp.where(row_lane < HALO, rims[(q + GZ - 1) % GZ], 0.0)
            )
        near = [lines[q, h * 32 : (h + 1) * 32, :] for q in range(GZ)]
        sums = jnp.concatenate([near[0] + near[2], near[1] + near[3]], 1)
        gaps = jnp.concatenate([near[0] - near[2], near[1] - near[3]], 1)
        even = dot3(halves(sums), (wz[0], wz[1]), NN)
        odd = dot3(halves(gaps), (wz[2], wz[3]), NN)
        for c in range(2):
            part = jnp.concatenate(
                [
                    v[:, p * 256 + c * 128 : p * 256 + (c + 1) * 128].reshape(HX, 8, 128)
                    for v in (even, odd)
                    for p in range(2)
                ],
                0,
            )
            out4[h, c * 16 : (c + 1) * 16] = swap_lanes(part, 16, 1)

        @unrolled(RING - 1)
        def _(i):
            copy4(h, ring_step(i), me).start()

        in4[h, pl.ds(pl.multiple_of(me * 8, 8), 8), :] = out4[h, me]

    dens_in[gz] = lines[gz]

    cosines = (wxy[0], wxy[1])
    sines = (wxy[2], wxy[3])
    real_lane = iota((NXY, 128), 1) // HX % 2 == 0
    for h in range(2):
        arrived(in4.at[h, 0 : NXY - 8], r4.at[h])

        rows_in = halves(in4[h])
        with_cos = dot3(cosines, rows_in, NN)
        with_sin = dot3(sines, rows_in, NN)
        out5[h] = with_cos + jnp.where(
            real_lane, pltpu.roll(with_sin, 128 - HX, 1), -pltpu.roll(with_sin, HX, 1)
        )

        @unrolled(GX - 1)
        def _(i):
            copy5(h, plane_step(i), gx).start()

        in5[h, gx] = out5[h, pl.ds(pl.multiple_of(gx * 8, 8), 8), :]

        if h == 0:
            copy_d(2 - 2 * half + core, gz).start()
            copy_d(3 - 2 * half - core, gz).start()
            copy_d(2 * half + 1 - core, gz).start()

    for h in range(2):
        arrived(in5.at[h, 0 : GX - 1], r5.at[h])
    arrived(dens_in.at[0 : GZ - 1], rd)
    arrived(out1.at[0 : GX - 1], s1)
    arrived(lines.at[0 : GZ - 1], sd)
    for h in range(2):
        arrived(out5.at[h, 0 : NXY - 8], s5.at[h])
        arrived(out4.at[h, 0 : RING - 1], s4.at[h])
        arrived(slabs.at[h, 0 : GROUPS - 1], s3.at[h])


def last_kernel(dens_in, in5, wx, dens_ref, spec_ref):
    with_cos = with_sin = None
    for h in range(2):
        x_lines = swap_lanes(in5[h], 32, HX).reshape(16, 2, 8, 128)
        x_lines = jnp.concatenate(
            [x_lines[:, p].reshape(128, 128) for p in range(2)], 0
        )
        x_lines = halves(x_lines)
        rows = slice(h * 128, (h + 1) * 128)
        add_cos = dot3(x_lines, (wx[0, rows], wx[1, rows]), NN)
        add_sin = dot3(x_lines, (wx[2, rows], wx[3, rows]), NN)
        with_cos = add_cos if h == 0 else with_cos + add_cos
        with_sin = add_sin if h == 0 else with_sin + add_sin
    spec_ref[0] = (with_cos[:128] + with_sin[128:]).reshape(16, 8, NXY)
    spec_ref[1] = (with_cos[128:] - with_sin[:128]).reshape(16, 8, NXY)
    for q in range(GZ):
        dens_ref[:, q * 8 : (q + 1) * 8, :] = dens_in[q].reshape(8, 8, 128)


def solution(mesh):
    wz = np.concatenate([np.stack(np_halves(m)) for m in depth_matrices()])
    wxy = np.concatenate([np.stack(np_halves(m)) for m in plane_matrices()])
    wxy, wx = wxy[:4], wxy[4:]
    vmem = pl.BlockSpec(memory_space=pltpu.VMEM)
    far = pl.BlockSpec(memory_space=pltpu.HBM)
    dma = pltpu.SemaphoreType.DMA
    call = pl.pallas_call(
        kernel,
        out_shape=(
            pltpu.VMEM((GZ, 64, 128), F32),
            pltpu.VMEM((2, GX, 8, 128), F32),
        ),
        in_specs=[far] * 6 + [pl.BlockSpec(memory_space=pltpu.SMEM), far, far],
        out_specs=(vmem, vmem),
        scratch_shapes=[
            pltpu.VMEM((32, 529), F32),
            pltpu.VMEM((NPOLY, 529), F32),
            pltpu.VMEM((3, 32), jnp.int32),
            pltpu.VMEM((3, 32), F32),
            pltpu.VMEM((1, 32), jnp.int32),
            pltpu.VMEM((1, 32), jnp.int32),
            pltpu.VMEM((4, NZ // 2, NZ), BF16),
            pltpu.VMEM((4, NXY, NXY), BF16),
            pltpu.VMEM((GX, 4, 128), F32),
            pltpu.VMEM((GX, 4, 128), F32),
            pltpu.VMEM((4 * GX, 128), F32),
            pltpu.VMEM((16, 8, SLOTS), F32),
            pltpu.VMEM((192, 4 * SLOTS), BF16),
            pltpu.VMEM((192, 4 * SLOTS), BF16),
            pltpu.VMEM((2, GROUPS, SLAB, 128), F32),
            pltpu.VMEM((2, GZ, SLAB, 128), F32),
            pltpu.VMEM((2, GZ, SLAB, 128), F32),
            pltpu.VMEM((GZ, 64, 128), F32),
            pltpu.VMEM((2, RING, 8, 128), F32),
            pltpu.VMEM((2, NXY, 128), F32),
            pltpu.VMEM((2, NXY, 128), F32),
            dma((8,)),
            dma, dma,
            dma((2,)), dma((2,)), dma((2,)),
            dma((2,)), dma((2,)),
            dma((2,)), dma((2,)),
            dma, dma,
        ],
        compiler_params=pltpu.CompilerParams(collective_id=0, has_side_effects=True),
        name="pair_grid_transform",
    )
    last = pl.pallas_call(
        last_kernel,
        out_shape=(
            jax.ShapeDtypeStruct((CX, CY, CZ), F32),
            jax.ShapeDtypeStruct((2, 16, 8, NXY), F32),
        ),
        in_specs=[vmem] * 3,
        out_specs=(vmem, vmem),
        compiler_params=pltpu.CompilerParams(vmem_limit_bytes=16 * 1024 * 1024),
        name="x_transform",
    )

    def shards(blocks, basis, cells, offsets, eidx, ridx, exps):
        dens, lines = call(
            blocks.T, basis.T, cells, offsets, eidx.reshape(1, -1), ridx.reshape(1, -1), exps,
            jnp.asarray(wz), jnp.asarray(wxy),
        )
        return last(dens, lines, jnp.asarray(wx))

    split = ("gx", "gy", "gz")
    placed = (P(None, split), P(), P(None, split), P(None, split), P(split), P(split), P())
    return jax.shard_map(
        shards,
        mesh=mesh,
        in_specs=placed,
        out_specs=(P("gx", "gy", "gz"), P(None, ("gy", "gz"), "gx", None)),
        check_vma=False,
    )
```
